256 devices in a mesh: gx: 8 (over y, x_hi), gy: 4 (over x_lo, core), gz: 8 (over z).
Axes of the slice: x: 4 (x_hi: 2, x_lo: 2; x = x_hi * 2 + x_lo), y: 4, z: 8, core: 2. Of those that a mesh axis runs over, the one named last changes fastest.
Arguments:
- coeffs: bfloat16 [8, 4, 8, 128, 3200], P('gx', 'gy', 'gz'), may hold values from -6 to 6
- halo_rows: int32 [8, 4, 8, 32], P('gx', 'gy', 'gz'), may hold values from 0 to 127
- edge_source: int32 [8, 4, 8, 4, 128], P('gx', 'gy', 'gz'), may hold values from 0 to 991
- edge_target: int32 [8, 4, 8, 4, 128], P('gx', 'gy', 'gz'), may hold values from 0 to 127
- edge_count: int32 [8, 4, 8, 4], P('gx', 'gy', 'gz'), may hold values from 1 to 128
- block_count: int32 [8, 4, 8], P('gx', 'gy', 'gz'), may hold values from 0 to 4, as said below
- wigner: bfloat16 [8, 4, 8, 4, 165, 128], P('gx', 'gy', 'gz'), may hold values from -2.6875 to 2.6875
- w_zero: bfloat16 [2, 640, 640], replicated, may hold values from -0.25 to 0.25
- w_one: bfloat16 [2, 2, 512, 512], replicated, may hold values from -0.1875 to 0.1875
- w_two: bfloat16 [2, 2, 384, 384], replicated, may hold values from -0.21875 to 0.21875
- attn_vector: float32 [128], replicated, may hold values from -3 to 3
Outputs:
- update: bfloat16 [8, 4, 8, 128, 3200], P('gx', 'gy', 'gz')
The draws below stay inside these ranges and needn't reach their ends.
Inputs may be any that keep to these rules, and one draw needn't show every extreme that they name: `edge_source`: rows of the home device's source table: 128 own atoms, then 27 blocks of 32. Devices 2i and 2i + 1 along gz (same gx and gy) hold 4 live blocks together; the live blocks of a home are its first block_count ones.
All inputs are finite; a program needn't handle non-finite values.
Results may differ from the reference program's by a relative error of at most 0.0079.
Values may be sent and summed in bfloat16 or wider, within the bound.
A program may use at most 128 MiB of HBM per device.

```python
import math
import jax
import jax.numpy as jnp
import numpy as np
from jax import lax

CH = 128
HEADS = 8
A_DEV = 128
BLOCK = 128
SLOTS = 2
HOMEB = 4
HB = 32
POOL = 992
N_GX = 8
N_GY = 4
N_GZ = 8


def draw_block_count(key, part):
    pairs = N_GX * N_GY * (N_GZ // 2)
    moved = jax.random.randint(jax.random.fold_in(key, 11), (pairs,), -SLOTS, SLOTS + 1)
    forced = jax.random.randint(jax.random.fold_in(key, 12), (), 0, pairs)
    direction = 2 * jax.random.randint(jax.random.fold_in(key, 13), (), 0, 2) - 1
    moved = jnp.where(jnp.arange(pairs) == forced, SLOTS * direction, moved)
    lower = SLOTS + moved
    upper = SLOTS - moved
    stacked = jnp.stack([lower, upper], axis=-1).reshape(N_GX, N_GY, N_GZ)
    return stacked.astype(jnp.int32)


def plant(drawn, stream_key, low, top_value):
    dims = drawn.shape
    spot = [jax.random.randint(jax.random.fold_in(stream_key, axis), (), 0, dims[axis]) for axis in range(len(dims))]
    drawn = drawn.at[tuple(spot)].set(low)
    longest = dims.index(max(dims))
    spot[longest] = (spot[longest] + 1) % dims[longest]
    return drawn.at[tuple(spot)].set(top_value)


def levels(stream_key, shape, cuts, least, top_value):
    level, own = 1.0, jax.random.fold_in(stream_key, 6)
    for axis_at, blocks in cuts:
        heights = jnp.exp(jax.random.uniform(jax.random.fold_in(own, axis_at), (blocks,), jnp.float32, least / len(cuts), top_value / len(cuts)))
        level = level * jnp.repeat(heights, shape[axis_at] // blocks).reshape([-1 if axis == axis_at else 1 for axis in range(len(shape))])
    return level


def noise(key, dims, spread, limit, cuts=(), kind=jnp.bfloat16):
    level = levels(key, dims, cuts, -0.22, 0.18) if cuts else 1.0
    drawn = jax.random.normal(key, dims, jnp.float32) * spread * level
    return jnp.minimum(jnp.maximum(drawn, -limit), limit).astype(kind)


def setup_inputs(seed: int = 0) -> dict:
    streams_of = jax.random.split(jax.random.key(seed), 12)
    coeffs = noise(streams_of[0], (N_GX, N_GY, N_GZ, A_DEV, 25 * CH), 1.0, 6.0, ((0, 8), (1, 4), (2, 8)))
    halo_rows = plant(jax.random.randint(streams_of[1], (N_GX, N_GY, N_GZ, HB), 0, A_DEV), jax.random.fold_in(streams_of[1], 1), 0, A_DEV - 1).astype(jnp.int32)
    edge_source = plant(jax.random.randint(streams_of[2], (N_GX, N_GY, N_GZ, HOMEB, BLOCK), 0, POOL), jax.random.fold_in(streams_of[2], 1), 0, POOL - 1).astype(jnp.int32)
    edge_target = plant(jax.random.randint(streams_of[3], (N_GX, N_GY, N_GZ, HOMEB, BLOCK), 0, A_DEV), jax.random.fold_in(streams_of[3], 1), 0, A_DEV - 1).astype(jnp.int32)
    edge_count = plant(jax.random.randint(streams_of[4], (N_GX, N_GY, N_GZ, HOMEB), 1, BLOCK + 1), jax.random.fold_in(streams_of[4], 1), 1, BLOCK).astype(jnp.int32)
    block_count = draw_block_count(jax.random.fold_in(streams_of[11], 71), 0)
    wigner = noise(streams_of[6], (N_GX, N_GY, N_GZ, HOMEB, 165, BLOCK), 0.45, 2.6875, ((0, 8), (1, 4), (2, 8)))
    w_zero = noise(streams_of[7], (2, 5 * CH, 5 * CH), (5 * CH) ** -0.5, 0.25)
    w_one = noise(streams_of[8], (2, 2, 4 * CH, 4 * CH), (8 * CH) ** -0.5, 0.1875)
    w_two = noise(streams_of[9], (2, 2, 3 * CH, 3 * CH), (6 * CH) ** -0.5, 0.21875)
    attn_vector = noise(streams_of[10], (CH,), 0.5, 3.0, (), jnp.float32)
    return dict(coeffs=coeffs, halo_rows=halo_rows, edge_source=edge_source, edge_target=edge_target, edge_count=edge_count, block_count=block_count, wigner=wigner, w_zero=w_zero, w_one=w_one, w_two=w_two, attn_vector=attn_vector)


EPS = 1e-06

def keep_index():
    ordering = [0, 2, 6, 12, 20, 3, 7, 13, 21, 1, 5, 11, 19, 8, 14, 22, 4, 10, 18]
    starts = [0, 1, 10, 35, 84]
    lookup = np.full((19, 25), 165, dtype=np.int32)
    for row_pos, component in enumerate(ordering):
        degree = math.isqrt(component)
        offset = component - degree * degree
        for column in range(2 * degree + 1):
            lookup[row_pos, degree * degree + column] = starts[degree] + offset * (2 * degree + 1) + column
    return lookup

def expand_frames(packed):
    padded = jnp.concatenate([packed, jnp.zeros_like(packed[:, :1])], axis=1)
    picked = jnp.take(padded, jnp.asarray(keep_index().reshape(-1)), axis=1)
    return picked.reshape(packed.shape[0], 19, 25, packed.shape[2])

def rms_norm(values):
    widened = values.astype(jnp.float32)
    factor = lax.rsqrt(lax.optimization_barrier(jnp.mean(widened * widened, axis=-1, keepdims=True)) + EPS)
    return (widened * factor).astype(jnp.bfloat16)

def product(left, right):
    return jnp.dot(left, right, preferred_element_type=jnp.float32)

def degree_mix(inputs, weight_zero, weight_one, weight_two):
    zero_out = product(inputs[:, :5 * CH], weight_zero)
    plus_one = inputs[:, 5 * CH:9 * CH]
    minus_one = inputs[:, 9 * CH:13 * CH]
    plus_two = inputs[:, 13 * CH:16 * CH]
    minus_two = inputs[:, 16 * CH:]
    one_plus = product(plus_one, weight_one[0]) - product(minus_one, weight_one[1])
    one_minus = product(minus_one, weight_one[0]) + product(plus_one, weight_one[1])
    two_plus = product(plus_two, weight_two[0]) - product(minus_two, weight_two[1])
    two_minus = product(minus_two, weight_two[0]) + product(plus_two, weight_two[1])
    return jnp.concatenate([zero_out, one_plus, one_minus, two_plus, two_minus], axis=1)

def edge_work(rotated, live_mask, w_zero, w_one, w_two, attn_vector):
    edge_total = rotated.shape[0]
    mixed_one = degree_mix(rotated, w_zero[0], w_one[0], w_two[0])
    scalars = mixed_one[:, :CH]
    logits = lax.optimization_barrier(jnp.sum((jax.nn.silu(scalars) * attn_vector).reshape(edge_total, HEADS, CH // HEADS), axis=-1))
    weights = jax.nn.sigmoid(logits) * live_mask[:, None]
    higher = mixed_one[:, CH:].reshape(edge_total, 18, CH) * jax.nn.sigmoid(scalars)[:, None, :]
    activated = jnp.concatenate([jax.nn.silu(scalars), higher.reshape(edge_total, 18 * CH)], axis=1).astype(jnp.bfloat16)
    mixed_two = degree_mix(activated, w_zero[1], w_one[1], w_two[1])
    weighted = mixed_two.reshape(edge_total, 19, HEADS, CH // HEADS) * weights[:, None, :, None]
    return weighted.reshape(edge_total, 19 * CH).astype(jnp.bfloat16)

def reference(coeffs, halo_rows, edge_source, edge_target, edge_count, block_count, wigner, w_zero, w_one, w_two, attn_vector):
    feature_width = 25 * CH
    normed = rms_norm(coeffs)
    boundary = jnp.take_along_axis(normed, halo_rows[..., None], axis=3)

    def device(flat_id):
        grid_x = flat_id // (N_GY * N_GZ)
        grid_y = flat_id // N_GZ % N_GY
        grid_z = flat_id % N_GZ
        pieces = [normed[grid_x, grid_y, grid_z]]
        for step_x in (-1, 0, 1):
            for step_y in (-1, 0, 1):
                for step_z in (-1, 0, 1):
                    pieces.append(boundary[(grid_x + step_x) % N_GX, (grid_y + step_y) % N_GY, (grid_z + step_z) % N_GZ])
        source_table = jnp.concatenate(pieces, axis=0)
        sources = edge_source[grid_x, grid_y, grid_z]
        targets = edge_target[grid_x, grid_y, grid_z]
        counts = edge_count[grid_x, grid_y, grid_z]
        owned = block_count[grid_x, grid_y, grid_z]
        frames = expand_frames(wigner[grid_x, grid_y, grid_z]).astype(jnp.float32)
        gathered = source_table[sources.reshape(-1)].reshape(HOMEB, BLOCK, 25, CH).astype(jnp.float32)
        rotated = jnp.einsum('gije,gejc->geic', frames, gathered).astype(jnp.bfloat16)
        edge_pos = jnp.arange(BLOCK, dtype=jnp.int32)[None, :]
        block_pos = jnp.arange(HOMEB, dtype=jnp.int32)[:, None]
        live_mask = ((edge_pos < counts[:, None]) & (block_pos < owned)).astype(jnp.float32).reshape(-1)
        weighted = edge_work(rotated.reshape(HOMEB * BLOCK, 19 * CH), live_mask, w_zero, w_one, w_two, attn_vector)
        weighted = weighted.reshape(HOMEB, BLOCK, 19, CH).astype(jnp.float32)
        message = jnp.einsum('gije,geic->gejc', frames, weighted).astype(jnp.bfloat16)
        summed = jnp.zeros((A_DEV, feature_width), jnp.float32)
        summed = summed.at[targets.reshape(-1)].add(message.reshape(HOMEB * BLOCK, feature_width).astype(jnp.float32))
        return summed.astype(jnp.bfloat16)
    result = lax.map(device, jnp.arange(N_GX * N_GY * N_GZ, dtype=jnp.int32))
    return result.reshape(N_GX, N_GY, N_GZ, A_DEV, feature_width)
```

```python
import math
import functools
import jax, jax.numpy as jnp, numpy as np
from jax import lax
from jax.experimental import pallas as pl
from jax.experimental.pallas import tpu as pltpu
from jax.sharding import PartitionSpec as P

CH = 128
F32 = jnp.float32
BF16 = jnp.bfloat16
STARTS = [0, 1, 10, 35, 84]
ORDER = [0, 2, 6, 12, 20, 3, 7, 13, 21, 1, 5, 11, 19, 8, 14, 22, 4, 10, 18]
ROWS = []
for l in range(5):
    rows = []
    for pos, comp in enumerate(ORDER):
        if math.isqrt(comp) == l:
            off = comp - l * l
            rows.append((pos, [STARTS[l] + off * (2 * l + 1) + j for j in range(2 * l + 1)]))
    ROWS.append(rows)
USED = sorted({p for rows in ROWS for _, ps in rows for p in ps})
SLOT = {p: i for i, p in enumerate(USED)}
NE = 512


def bcast_frames(wig_ref, wb):
    for g in range(4):
        for i, p in enumerate(USED):
            row = wig_ref[g, p:p + 1, :].astype(F32)
            wb[i, :, g * 128:(g + 1) * 128] = jnp.broadcast_to(row, (8, 128))


def build_weights(wz, w1, w2, wzt, w1t, w2t):
    for v in range(2):
        for a in range(5):
            for b in range(5):
                wzt[v, b * CH:(b + 1) * CH, a * CH:(a + 1) * CH] = wz[v, a * CH:(a + 1) * CH, b * CH:(b + 1) * CH].T
        for (src, dst, n) in ((w1, w1t, 4), (w2, w2t, 3)):
            for a in range(n):
                for b in range(n):
                    re = src[v, 0, a * CH:(a + 1) * CH, b * CH:(b + 1) * CH].T
                    im = src[v, 1, a * CH:(a + 1) * CH, b * CH:(b + 1) * CH].T
                    dst[v, b * CH:(b + 1) * CH, a * CH:(a + 1) * CH] = re
                    dst[v, (n + b) * CH:(n + b + 1) * CH, (n + a) * CH:(n + a + 1) * CH] = re
                    dst[v, b * CH:(b + 1) * CH, (n + a) * CH:(n + a + 1) * CH] = -im
                    dst[v, (n + b) * CH:(n + b + 1) * CH, a * CH:(a + 1) * CH] = im


def transpose_table(tab, tabt):
    def step(k, _):
        c = pl.multiple_of(k * 128, 128)
        for g in range(8):
            tabt[pl.ds(c, 128), g * 128:(g + 1) * 128] = tab[g * 128:(g + 1) * 128, pl.ds(c, 128)].T
        return 0
    lax.fori_loop(0, 25, step, 0)


def rotate_in(l, gl, wb, rot):
    d = 2 * l + 1
    def step(it, _):
        e = pl.multiple_of((it % 4) * 128, 128)
        c = pl.multiple_of((it // 4) * 16, 16)
        outs = [[], [], [], [], []]
        for h in range(2):
            g = [gl[pl.ds(j * CH + c + 8 * h, 8), pl.ds(e, 128)] for j in range(d)]
            for n, (pos, ps) in enumerate(ROWS[l]):
                acc = None
                for j in range(d):
                    t = wb[SLOT[ps[j]], :, pl.ds(e, 128)] * g[j]
                    acc = t if acc is None else acc + t
                outs[n].append(acc)
        for n, (pos, ps) in enumerate(ROWS[l]):
            rot[pl.ds(pos * CH + c, 16), pl.ds(e, 128)] = jnp.concatenate(outs[n], axis=0).astype(BF16)
        return 0
    lax.fori_loop(0, 32, step, 0)


def rotate_out(l, wei, wb, msg):
    d = 2 * l + 1
    def step(it, _):
        e = pl.multiple_of((it % 4) * 128, 128)
        c = pl.multiple_of((it // 4) * 16, 16)
        w = [wei[pl.ds(pos * CH + c, 16), pl.ds(e, 128)].astype(F32) for pos, _ in ROWS[l]]
        for j in range(d):
            halves = []
            for h in range(2):
                acc = None
                for n, (pos, ps) in enumerate(ROWS[l]):
                    t = wb[SLOT[ps[j]], :, pl.ds(e, 128)] * w[n][8 * h:8 * h + 8]
                    acc = t if acc is None else acc + t
                halves.append(acc)
            msg[pl.ds(j * CH + c, 16), pl.ds(e, 128)] = jnp.concatenate(halves, axis=0).astype(BF16)
        return 0
    lax.fori_loop(0, 32, step, 0)


def dot(a, b):
    return jnp.dot(a, b, preferred_element_type=F32)


def conv_parts(v, x, wzt, w1t, w2t, emit):
    emit(0, 1, dot(wzt[v, 0:128, :], x[0:640, :]))
    emit(1, 2, dot(wzt[v, 128:384, :], x[0:640, :]))
    emit(3, 2, dot(wzt[v, 384:640, :], x[0:640, :]))
    for b in range(4):
        emit(5 + 2 * b, 2, dot(w1t[v, b * 256:(b + 1) * 256, :], x[640:1664, :]))
    for b in range(3):
        emit(13 + 2 * b, 2, dot(w2t[v, b * 256:(b + 1) * 256, :], x[1664:2432, :]))


def compute(src, tgt, cnt, blocks, attn_ref, tabt, wb, wzt, w1t, w2t, rowid, out, oh, gl, rot, act, wei, msg, attb, sigs):
    for g in range(4):
        oh[:, g * 128:(g + 1) * 128] = jnp.where(rowid == src[g:g + 1, :], 1.0, 0.0).astype(BF16)
    for l in range(5):
        d = 2 * l + 1
        for j in range(d):
            gl[j * CH:(j + 1) * CH, :] = dot(tabt[(l * l + j) * CH:(l * l + j + 1) * CH, :], oh[...])
        rotate_in(l, gl, wb, rot)

    attn = jnp.broadcast_to(attn_ref[...].reshape(1, 128), (128, 128)).T

    def emit1(c0, n, val):
        if c0 == 0:
            sig = jax.nn.sigmoid(val)
            sigs[...] = sig
            silu = val * sig
            act[0:128, :] = silu.astype(BF16)
            for g in range(4):
                t = (silu[:, g * 128:(g + 1) * 128] * attn).reshape(8, 16, 128)
                logit = jnp.sum(t, axis=1)
                edge = lax.broadcasted_iota(jnp.int32, (8, 128), 1)
                live = jnp.logical_and(edge < cnt[g], g < blocks)
                a = jnp.where(live, jax.nn.sigmoid(logit), 0.0)
                attb[:, g * 128:(g + 1) * 128] = jnp.broadcast_to(a[:, None, :], (8, 16, 128)).reshape(128, 128)
        else:
            for k in range(n):
                act[(c0 + k) * CH:(c0 + k + 1) * CH, :] = (val[k * CH:(k + 1) * CH] * sigs[...]).astype(BF16)
    conv_parts(0, rot, wzt, w1t, w2t, emit1)

    def emit2(c0, n, val):
        for k in range(n):
            wei[(c0 + k) * CH:(c0 + k + 1) * CH, :] = (val[k * CH:(k + 1) * CH] * attb[...]).astype(BF16)
    conv_parts(1, act, wzt, w1t, w2t, emit2)

    ot = []
    for g in range(4):
        atom = lax.broadcasted_iota(jnp.int32, (128, 128), 0)
        ot.append(jnp.where(atom == tgt[g:g + 1, :], 1.0, 0.0).astype(BF16))
    ot = jnp.concatenate(ot, axis=1)
    for l in range(5):
        d = 2 * l + 1
        rotate_out(l, wei, wb, msg)
        upd = lax.dot_general(ot, msg[0:d * CH, :], (((1,), (1,)), ((), ())), preferred_element_type=F32)
        out[:, l * l * CH:(l + 1) * (l + 1) * CH] = upd.astype(BF16)


COMPUTE_SCRATCH = [
    pltpu.VMEM((1024, NE), BF16),
    pltpu.VMEM((9 * CH, NE), F32),
    pltpu.VMEM((19 * CH, NE), BF16),
    pltpu.VMEM((19 * CH, NE), BF16),
    pltpu.VMEM((19 * CH, NE), BF16),
    pltpu.VMEM((9 * CH, NE), BF16),
    pltpu.VMEM((CH, NE), F32),
    pltpu.VMEM((CH, NE), F32),
]
PREP_SCRATCH = [
    pltpu.VMEM((3200, 1024), BF16),
    pltpu.VMEM((115, 8, NE), F32),
    pltpu.VMEM((2, 640, 640), BF16),
    pltpu.VMEM((2, 1024, 1024), BF16),
    pltpu.VMEM((2, 768, 768), BF16),
]


def v1_kernel(cnt, blocks, tab, src, tgt, wig, wz, w1, w2, attn, out, tabt, wb, wzt, w1t, w2t, tabp, *scr):
    bcast_frames(wig, wb)
    build_weights(wz, w1, w2, wzt, w1t, w2t)
    tabp[0:992, :] = tab[...]
    tabp[992:1024, :] = jnp.zeros((32, 3200), BF16)
    transpose_table(tabp, tabt)
    rowid = lax.broadcasted_iota(jnp.int32, (1024, 1), 0)
    compute(src, tgt, cnt, blocks[0], attn, tabt, wb, wzt, w1t, w2t, rowid, out, *scr)


def v1_call(tab, src, tgt, cnt, blocks, wig, wz, w1, w2, attn):
    vm = pl.BlockSpec(memory_space=pltpu.VMEM)
    sm = pl.BlockSpec(memory_space=pltpu.SMEM)
    return pl.pallas_call(
        v1_kernel,
        out_shape=jax.ShapeDtypeStruct((128, 3200), BF16),
        in_specs=[sm, sm] + [vm] * 8,
        out_specs=vm,
        scratch_shapes=PREP_SCRATCH + [pltpu.VMEM((1024, 3200), BF16)] + COMPUTE_SCRATCH,
        compiler_params=pltpu.CompilerParams(vmem_limit_bytes=67043328),
    )(cnt, blocks, tab, src, tgt, wig, wz, w1, w2, attn.reshape(1, 128))


EPS = 1e-06


def with_halo(block, sides, width):
    for axis, dim in sides:
        count = lax.axis_size(axis)
        forward = [(i, (i + 1) % count) for i in range(count)]
        backward = [(target, source) for source, target in forward]
        low = lax.ppermute(lax.slice_in_dim(block, block.shape[dim] - width, None, axis=dim), axis, forward)
        high = lax.ppermute(lax.slice_in_dim(block, 0, width, axis=dim), axis, backward)
        block = jnp.concatenate([low, block, high], axis=dim)
    return block


def body(coeffs, halo_rows, edge_source, edge_target, edge_count, block_count, wigner, w_zero, w_one, w_two, attn_vector):
    width = coeffs.shape[4]
    wide = coeffs[0, 0, 0].astype(F32)
    normed = (wide * lax.rsqrt(jnp.mean(wide * wide, axis=-1, keepdims=True) + EPS)).astype(BF16)
    boundary = normed[halo_rows[0, 0, 0]]
    received = with_halo(boundary[None, None, None], (("gx", 0), ("gy", 1), ("gz", 2)), 1)
    table = jnp.concatenate([normed, received.reshape(-1, width)], axis=0)
    out = v1_call(table, edge_source[0, 0, 0], edge_target[0, 0, 0], edge_count[0, 0, 0], block_count[0, 0],
                  wigner[0, 0, 0], w_zero, w_one, w_two, attn_vector)
    return out.reshape(1, 1, 1, 128, width)


def solution(mesh):
    placed = (P("gx", "gy", "gz", None, None), P("gx", "gy", "gz", None), P("gx", "gy", "gz", None, None), P("gx", "gy", "gz", None, None),
              P("gx", "gy", "gz", None), P("gx", "gy", "gz"), P("gx", "gy", "gz", None, None, None), P(), P(), P(), P())
    return jax.shard_map(body, mesh=mesh, in_specs=placed, out_specs=P("gx", "gy", "gz", None, None), check_vma=False)
```

```python
import math
import functools
import jax, jax.numpy as jnp, numpy as np
from jax import lax
from jax.experimental import pallas as pl
from jax.experimental.pallas import tpu as pltpu
from jax.sharding import PartitionSpec as P

CH = 128
F32 = jnp.float32
BF16 = jnp.bfloat16
STARTS = [0, 1, 10, 35, 84]
ORDER = [0, 2, 6, 12, 20, 3, 7, 13, 21, 1, 5, 11, 19, 8, 14, 22, 4, 10, 18]
ROWS = []
for l in range(5):
    rows = []
    for pos, comp in enumerate(ORDER):
        if math.isqrt(comp) == l:
            off = comp - l * l
            rows.append((pos, [STARTS[l] + off * (2 * l + 1) + j for j in range(2 * l + 1)]))
    ROWS.append(rows)
USED = sorted({p for rows in ROWS for _, ps in rows for p in ps})
SLOT = {p: i for i, p in enumerate(USED)}
NE = 512


def rotate_out(l, wei, wb, msg):
    d = 2 * l + 1
    def step(it, _):
        e = pl.multiple_of((it % 4) * 128, 128)
        c = pl.multiple_of((it // 4) * 16, 16)
        w = [wei[pl.ds(pos * CH + c, 16), pl.ds(e, 128)].astype(F32) for pos, _ in ROWS[l]]
        for j in range(d):
            halves = []
            for h in range(2):
                acc = None
                for n, (pos, ps) in enumerate(ROWS[l]):
                    t = wb[SLOT[ps[j]], :, pl.ds(e, 128)] * w[n][8 * h:8 * h + 8]
                    acc = t if acc is None else acc + t
                halves.append(acc)
            msg[pl.ds(j * CH + c, 16), pl.ds(e, 128)] = jnp.concatenate(halves, axis=0).astype(BF16)
        return 0
    lax.fori_loop(0, 32, step, 0)


def dot(a, b):
    return jnp.dot(a, b, preferred_element_type=F32)


def conv_parts(v, x, wzt, w1t, w2t, emit):
    emit(0, 1, dot(wzt[v, 0:128, :], x[0:640, :]))
    emit(1, 2, dot(wzt[v, 128:384, :], x[0:640, :]))
    emit(3, 2, dot(wzt[v, 384:640, :], x[0:640, :]))
    for b in range(4):
        emit(5 + 2 * b, 2, dot(w1t[v, b * 256:(b + 1) * 256, :], x[640:1664, :]))
    for b in range(3):
        emit(13 + 2 * b, 2, dot(w2t[v, b * 256:(b + 1) * 256, :], x[1664:2432, :]))


P_S, P_O, P_YO, P_L, P_R, P_YC = range(6)
LINKS = ("right", "left", "yt", "zp", "zm", "partner")
CHUNKS = ((16, 5, "B"), (21, 4, "A"), (9, 4, "B"), (13, 3, "A"), (0, 5, "B"), (5, 4, "A"))
GROUPS = (((0, 1), (4,)), ((2, 3), (3,)), ((4, 5), (2, 1, 0)))


def geometry(gx, gy, gz, div, rem):
    y, xh, xl, c = div(gx, 2), rem(gx, 2), div(gy, 2), rem(gy, 2)
    xor = lambda a, b: a + b - 2 * a * b
    dev = dict(
        right=(y * 2 + xor(xh, xl), 2 * (1 - xl) + c, gz),
        left=(y * 2 + xor(xh, 1 - xl), 2 * (1 - xl) + c, gz),
        yt=(rem(y + 5 - 2 * xh, 4) * 2 + xh, gy, gz),
        ys=(rem(y + 3 + 2 * xh, 4) * 2 + xh, gy, gz),
        zp=(gx, gy, rem(gz + 1, 8)),
        zm=(gx, gy, rem(gz + 7, 8)),
        partner=(gx, 2 * xl + 1 - c, gz),
    )
    dev["relay"] = tuple(a * (1 - c) + b * c for a, b in zip(dev["right"], dev["left"]))
    s, t = 1 - 2 * xh, 1 - 2 * c
    blocks = []
    for q in range(27):
        if q < 9:
            da, db = (0, s, -s)[q // 3], 0
        else:
            p = (q - 9) // 3
            da = (0, s, -s, (1 - xl) * s, xl * s, -s)[p]
            db = (t, t, t, -t, -t, -t)[p]
        blocks.append((da + 1) * 9 + (db + 1) * 3 + q % 3)
    return dev, c, xl, blocks


def chunk_ops(k, route):
    ops = []
    S, O, YO, L, R, YC = (3 * p for p in range(6))
    dks = (1, 0, 2) if route == "A" else (1,)
    if route == "A":
        ops.append((k, "zp", S + 1, S + 0, ()))
        ops.append((k, "zm", S + 1, S + 2, ()))
    for d in dks:
        pre = () if d == 1 else ((k, S + d),)
        ops.append((k, "right", S + d, L + d, pre))
        ops.append((k, "left", S + d, R + d, pre))
    for d in dks:
        ops.append((k, "relay", "F%d" % d, O + d, ((k, L + d), (k, R + d))))
    for d in dks:
        ops.append((k, "yt", "C%d" % d, YC + d, ((k, L + d), (k, R + d))))
        ops.append((k, "yt", O + d, YO + d, ((k, O + d),)))
    if route == "B":
        for p in range(6):
            pre = () if p == 0 else ((k, 3 * p + 1),)
            ops.append((k, "zp", 3 * p + 1, 3 * p + 0, pre))
            ops.append((k, "zm", 3 * p + 1, 3 * p + 2, pre))
    for p in range(6):
        pre = tuple((k, 3 * p + d) for d in range(3) if not (p == 0 and d == 1))
        ops.append((k, "partner", 3 * p, 100 + 3 * p, pre))
    return ops


def plan(pieces, lat=1.9, rate=46.6e3):
    ops = [op for k, (_, _, r) in enumerate(CHUNKS) for op in chunk_ops(k, r)]
    pend, free, arrive, seq, now = list(ops), {}, {}, [], 0.0
    pieces = list(pieces)

    def group_ready(g):
        if g < 0:
            return 0.0
        keys = [(k, 100 + 3 * p) for k in GROUPS[g][0] for p in range(6)]
        return max(arrive.get(key, 1e9) for key in keys)

    while pend or pieces:
        ready = [op for op in pend if all(arrive.get(x, 1e9) <= now for x in op[4])]
        if ready:
            op = ready[0]
            pend.remove(op)
            seq.append(("op", op))
            k, link, _, dst, _ = op
            size = 32 * CHUNKS[k][1] * 256 * (3 if link == "partner" else 1)
            lk = "right" if link == "relay" else link
            r = 300e3 if link == "partner" else rate * (1.33 if lk == "right" else 1.0)
            start = max(now, free.get(lk, 0.0))
            free[lk] = start + size / r
            arrive[(k, dst)] = free[lk] + (1.0 if link == "partner" else lat)
            now += 0.02
            continue
        if pieces and group_ready(pieces[0][2]) <= now:
            name, us, _ = pieces.pop(0)
            seq.append(("piece", name))
            now += us
            continue
        times = [max([arrive.get(x, 1e9) for x in op[4]]) for op in pend]
        if pieces:
            times.append(group_ready(pieces[0][2]))
        now = max(now, min(times))
    return seq, now, arrive

EPS = 1e-06
NK = len(CHUNKS)


def make_pieces():
    pieces = [("own", 1.0, -1), ("onehot", 0.5, -1)]
    pieces += [("frames%d" % g, 0.35, -1) for g in range(4)]
    pieces += [("weights%d" % i, 0.35, -1) for i in range(10)]
    for gi, (_, degrees) in enumerate(GROUPS):
        lo, hi = degrees[-1] ** 2, (degrees[0] + 1) ** 2
        step = 3 if gi == len(GROUPS) - 1 else 1
        j = lo
        while j < hi:
            n = min(step, hi - j)
            pieces.append(("gather%d:%d:%d:%d" % (gi, j, n, lo), 0.28 * n, gi))
            j += n
        for l in degrees:
            for e in range(4):
                pieces.append(("rotate%d:%d:%d" % (l, e, lo), 0.01 + 0.016 * (2 * l + 1) * min(5, 2 * l + 1) / 2, gi))
    return pieces


def rotate_tile(l, e, base, gl, wb, rot):
    d = 2 * l + 1
    e0 = e * 128

    def step(it, _):
        c = pl.multiple_of(it * 16, 16)
        outs = [[] for _ in ROWS[l]]
        for h in range(2):
            g = [gl[pl.ds((base + j) * CH + c + 8 * h, 8), e0:e0 + 128] for j in range(d)]
            for n, (pos, ps) in enumerate(ROWS[l]):
                acc = None
                for j in range(d):
                    t = wb[SLOT[ps[j]], :, e0:e0 + 128] * g[j]
                    acc = t if acc is None else acc + t
                outs[n].append(acc)
        for n, (pos, ps) in enumerate(ROWS[l]):
            rot[pl.ds(pos * CH + c, 16), e0:e0 + 128] = jnp.concatenate(outs[n], axis=0).astype(BF16)
        return 0

    lax.fori_loop(0, 8, step, 0)


def weight_blocks():
    todo = []
    for v in range(2):
        todo += [(v, 0, a, b) for a in range(5) for b in range(5)]
        todo += [(v, 1, a, b) for a in range(4) for b in range(4)]
        todo += [(v, 2, a, b) for a in range(3) for b in range(3)]
    return todo


def build_block(v, m, a, b, raw, built):
    src, dst, n = raw[m], built[m], (5, 4, 3)[m]
    ra, rb = slice(a * CH, (a + 1) * CH), slice(b * CH, (b + 1) * CH)
    if m == 0:
        dst[v, rb, ra] = src[v, ra, rb].T
        return
    hb, ha = slice((n + b) * CH, (n + b + 1) * CH), slice((n + a) * CH, (n + a + 1) * CH)
    re, im = src[v, 0, ra, rb].T, src[v, 1, ra, rb].T
    dst[v, rb, ra] = re
    dst[v, hb, ha] = re
    dst[v, rb, ha] = -im
    dst[v, hb, ra] = im


def merged_kernel(cnt, blocks, src4, tgt4, halo, attn, coeffs, wig_h, wz_h, w1_h, w2_h, out,
                  cf, wig, wzr, w1r, w2r, tab, tabo, tabt, wb, wzt, w1t, w2t,
                  oh, gl, rot, act, wei, msg, attb, sigs, lsem, ssem, rsem):
    MESH = pl.DeviceIdType.MESH
    gx, gy, gz = (lax.axis_index(n) for n in ("gx", "gy", "gz"))
    dev, core, xl, bids = geometry(gx, gy, gz, lax.div, lax.rem)
    src, tgt = src4.at[0, 0, 0], tgt4.at[0, 0, 0]

    loads = [pltpu.make_async_copy(a, b, lsem.at[i]) for i, (a, b) in enumerate(
        ((coeffs.at[0, 0, 0], cf), (wig_h.at[0, 0, 0], wig), (wz_h, wzr), (w1_h, w1r), (w2_h, w2r)))]
    for cp in loads:
        cp.start()
    barrier = pltpu.get_barrier_semaphore()
    near = ("right", "left", "yt", "ys", "zp", "zm", "partner")
    for n in near:
        pl.semaphore_signal(barrier, inc=1, device_id=dev[n], device_id_type=MESH)

    pick = jnp.where(lax.broadcasted_iota(jnp.int32, (128, 32), 0) == halo[0, 0], 1.0, 0.0).astype(F32).T.astype(BF16)
    loads[0].wait()
    rows = dot(pick, cf[...])
    rows = rows * lax.rsqrt(jnp.mean(rows * rows, axis=-1, keepdims=True) + EPS)
    tab[32:64, :] = rows.astype(BF16)
    tab[864:896, :] = jnp.zeros((32, 3200), BF16)
    pl.semaphore_wait(barrier, len(near))

    descs = {}

    def issue(op):
        k, link, s, d, _ = op
        j0, n, _ = CHUNKS[k]
        cols = pl.ds(j0 * CH, n * CH)
        cnt_slots = 3 if link == "partner" else 1
        if isinstance(s, str):
            sel = core if s[0] == "F" else xl
            row = pl.multiple_of((3 * sel + int(s[1])) * 32, 32)
            sref = tabo.at[pl.ds(row, 32), cols]
        elif s < 9:
            sref = tab.at[pl.ds(32 * s, 32 * cnt_slots), cols]
        else:
            sref = tabo.at[pl.ds(32 * (s - 9), 32 * cnt_slots), cols]
        if d >= 100:
            dref = tab.at[pl.ds(288 + 32 * (d - 100), 96), cols]
        elif d < 9:
            dref = tab.at[pl.ds(32 * d, 32), cols]
        else:
            dref = tabo.at[pl.ds(32 * (d - 9), 32), cols]
        i = len(descs)
        cp = pltpu.make_async_remote_copy(src_ref=sref, dst_ref=dref, send_sem=ssem.at[i], recv_sem=rsem.at[i],
                                          device_id=dev[link], device_id_type=MESH)
        descs[(k, d)] = cp
        return cp

    waited = set()

    def arrive(key):
        if key not in waited:
            waited.add(key)
            descs[key].wait_recv()

    raw, built = (wzr, w1r, w2r), (wzt, w1t, w2t)
    wblocks = weight_blocks()

    def piece(name):
        if name == "own":
            x = cf[...].astype(F32)
            f = lax.rsqrt(jnp.mean(x * x, axis=-1, keepdims=True) + EPS)
            for j in range(25):
                tabt[j * CH:(j + 1) * CH, 0:128] = (cf[:, j * CH:(j + 1) * CH].astype(F32) * f).astype(BF16).T
        elif name == "onehot":
            own = lax.broadcasted_iota(jnp.int32, (128, 128), 0)
            for g in range(4):
                oh[0:128, g * 128:(g + 1) * 128] = jnp.where(own == src[g:g + 1, :], 1.0, 0.0).astype(BF16)
                for q in range(27):
                    at = lax.broadcasted_iota(jnp.int32, (32, 128), 0) + (128 + 32 * bids[q])
                    oh[128 + 32 * q:160 + 32 * q, g * 128:(g + 1) * 128] = jnp.where(at == src[g:g + 1, :], 1.0, 0.0).astype(BF16)
                oh[992:1024, g * 128:(g + 1) * 128] = jnp.zeros((32, 128), BF16)
        elif name.startswith("frames"):
            g = int(name[6:])
            if g == 0:
                loads[1].wait()
            for i, p in enumerate(USED):
                wb[i, :, g * 128:(g + 1) * 128] = jnp.broadcast_to(wig[g, p:p + 1, :].astype(F32), (8, 128))
        elif name.startswith("weights"):
            i = int(name[7:])
            if i == 0:
                for cp in loads[2:]:
                    cp.wait()
            for blk in wblocks[i * 10:(i + 1) * 10]:
                build_block(*blk, raw, built)
        elif name.startswith("gather"):
            gi, j0, n, lo = (int(v) for v in name[6:].split(":"))
            for j in range(j0, j0 + n):
                for g in range(7):
                    tabt[j * CH:(j + 1) * CH, 128 + g * 128:256 + g * 128] = tab[g * 128:(g + 1) * 128, j * CH:(j + 1) * CH].T
            gl[(j0 - lo) * CH:(j0 - lo + n) * CH, :] = dot(tabt[j0 * CH:(j0 + n) * CH, :], oh[...])
        elif name.startswith("rotate"):
            l, e, lo = (int(v) for v in name[6:].split(":"))
            rotate_tile(l, e, l * l - lo, gl, wb, rot)

    got = set()
    seq, _, _ = plan(make_pieces())
    for kind, what in seq:
        if kind == "op":
            for key in what[4]:
                arrive(key)
            issue(what).start()
        else:
            if what[:6] == "gather":
                g = int(what[6:].split(":")[0])
                if g not in got:
                    got.add(g)
                    for k in GROUPS[g][0]:
                        for p in range(6):
                            arrive((k, 100 + 3 * p))
            piece(what)
    for key, cp in descs.items():
        arrive(key)
        cp.wait_send()

    finish(tgt, cnt, blocks, attn, wb, wzt, w1t, w2t, out, rot, act, wei, msg, attb, sigs)


def finish(tgt, cnt, blocks, attn_ref, wb, wzt, w1t, w2t, out, rot, act, wei, msg, attb, sigs):
    attn = jnp.broadcast_to(attn_ref[...], (128, 128)).T

    def emit1(c0, n, val):
        if c0 == 0:
            sig = jax.nn.sigmoid(val)
            sigs[...] = sig
            silu = val * sig
            act[0:128, :] = silu.astype(BF16)
            for g in range(4):
                t = (silu[:, g * 128:(g + 1) * 128] * attn).reshape(8, 16, 128)
                logit = jnp.sum(t, axis=1)
                edge = lax.broadcasted_iota(jnp.int32, (8, 128), 1)
                live = jnp.logical_and(edge < cnt[0, 0, 0, g], g < blocks[0, 0, 0])
                a = jnp.where(live, jax.nn.sigmoid(logit), 0.0)
                attb[:, g * 128:(g + 1) * 128] = jnp.broadcast_to(a[:, None, :], (8, 16, 128)).reshape(128, 128)
        else:
            for k in range(n):
                act[(c0 + k) * CH:(c0 + k + 1) * CH, :] = (val[k * CH:(k + 1) * CH] * sigs[...]).astype(BF16)
    conv_parts(0, rot, wzt, w1t, w2t, emit1)

    def emit2(c0, n, val):
        for k in range(n):
            wei[(c0 + k) * CH:(c0 + k + 1) * CH, :] = (val[k * CH:(k + 1) * CH] * attb[...]).astype(BF16)
    conv_parts(1, act, wzt, w1t, w2t, emit2)

    ot = []
    for g in range(4):
        atom = lax.broadcasted_iota(jnp.int32, (128, 128), 0)
        ot.append(jnp.where(atom == tgt[g:g + 1, :], 1.0, 0.0).astype(BF16))
    ot = jnp.concatenate(ot, axis=1)
    for l in range(5):
        d = 2 * l + 1
        rotate_out(l, wei, wb, msg)
        upd = lax.dot_general(ot, msg[0:d * CH, :], (((1,), (1,)), ((), ())), preferred_element_type=F32)
        out[0, 0, 0, :, l * l * CH:(l + 1) * (l + 1) * CH] = upd.astype(BF16)


def body(coeffs, halo_rows, edge_source, edge_target, edge_count, block_count, wigner, w_zero, w_one, w_two, attn_vector):
    vm = pl.BlockSpec(memory_space=pltpu.VMEM)
    sm = pl.BlockSpec(memory_space=pltpu.SMEM)
    hb = pl.BlockSpec(memory_space=pl.ANY)
    nops = sum(len(chunk_ops(k, r)) for k, (_, _, r) in enumerate(CHUNKS))
    V = pltpu.VMEM
    return pl.pallas_call(
        merged_kernel,
        out_shape=jax.ShapeDtypeStruct((1, 1, 1, 128, 3200), BF16),
        in_specs=[sm, sm, vm, vm, vm, vm, hb, hb, hb, hb, hb],
        out_specs=vm,
        scratch_shapes=[
            V((128, 3200), BF16), V((4, 165, 128), BF16), V((2, 640, 640), BF16), V((2, 2, 512, 512), BF16), V((2, 2, 384, 384), BF16),
            V((896, 3200), BF16), V((288, 3200), BF16), V((3200, 1024), BF16), V((115, 8, NE), F32),
            V((2, 640, 640), BF16), V((2, 1024, 1024), BF16), V((2, 768, 768), BF16),
            V((1024, NE), BF16), V((9 * CH, NE), F32), V((19 * CH, NE), BF16), V((19 * CH, NE), BF16), V((19 * CH, NE), BF16),
            V((9 * CH, NE), BF16), V((CH, NE), F32), V((CH, NE), F32),
            pltpu.SemaphoreType.DMA((5,)), pltpu.SemaphoreType.DMA((nops,)), pltpu.SemaphoreType.DMA((nops,)),
        ],
        compiler_params=pltpu.CompilerParams(vmem_limit_bytes=67043328, collective_id=0, has_side_effects=True),
    )(edge_count, block_count, edge_source, edge_target, halo_rows, attn_vector.reshape(1, 128), coeffs, wigner, w_zero, w_one, w_two)


def solution(mesh):
    placed = (P("gx", "gy", "gz", None, None), P("gx", "gy", "gz", None), P("gx", "gy", "gz", None, None), P("gx", "gy", "gz", None, None),
              P("gx", "gy", "gz", None), P("gx", "gy", "gz"), P("gx", "gy", "gz", None, None, None), P(), P(), P(), P())
    return jax.shard_map(body, mesh=mesh, in_specs=placed, out_specs=P("gx", "gy", "gz", None, None), check_vma=False)
```

```python
import math
import functools
import jax, jax.numpy as jnp, numpy as np
from jax import lax
from jax.experimental import pallas as pl
from jax.experimental.pallas import tpu as pltpu
from jax.sharding import PartitionSpec as P

CH = 128
F32 = jnp.float32
BF16 = jnp.bfloat16
STARTS = [0, 1, 10, 35, 84]
ORDER = [0, 2, 6, 12, 20, 3, 7, 13, 21, 1, 5, 11, 19, 8, 14, 22, 4, 10, 18]
ROWS = []
for l in range(5):
    rows = []
    for pos, comp in enumerate(ORDER):
        if math.isqrt(comp) == l:
            off = comp - l * l
            rows.append((pos, [STARTS[l] + off * (2 * l + 1) + j for j in range(2 * l + 1)]))
    ROWS.append(rows)
USED = sorted({p for rows in ROWS for _, ps in rows for p in ps})
SLOT = {p: i for i, p in enumerate(USED)}
NE = 512


def rotate_out(l, wei, wb, msg):
    d = 2 * l + 1
    for e in range(0, NE, 128):
        for c in range(0, CH, 16):
            w = [wei[pos * CH + c:pos * CH + c + 16, e:e + 128].astype(F32) for pos, _ in ROWS[l]]
            for j in range(d):
                acc = [None, None]
                for n, (pos, ps) in enumerate(ROWS[l]):
                    f = wb[SLOT[ps[j]], :, e:e + 128]
                    for h in range(2):
                        t = f * w[n][8 * h:8 * h + 8]
                        acc[h] = t if acc[h] is None else acc[h] + t
                r = (l * l + j) * CH + c
                msg[r:r + 16, e:e + 128] = jnp.concatenate(acc, axis=0).astype(BF16)


def dot(a, b):
    return jnp.dot(a, b, preferred_element_type=F32)


def conv_parts(v, x, wzt, w1t, w2t, emit):
    emit(0, 1, dot(wzt[v, 0:128, :], x[0:640, :]))
    emit(1, 2, dot(wzt[v, 128:384, :], x[0:640, :]))
    emit(3, 2, dot(wzt[v, 384:640, :], x[0:640, :]))
    for b in range(4):
        emit(5 + 2 * b, 2, dot(w1t[v, b * 256:(b + 1) * 256, :], x[640:1664, :]))
    for b in range(3):
        emit(13 + 2 * b, 2, dot(w2t[v, b * 256:(b + 1) * 256, :], x[1664:2432, :]))


P_S, P_O, P_YO, P_L, P_R, P_YC = range(6)
LINKS = ("right", "left", "yt", "zp", "zm", "partner")
CHUNKS = ((16, 5, "B"), (21, 4, "A"), (9, 4, "B"), (13, 3, "A"), (4, 3, "B"), (7, 2, "A"), (0, 2, "B"), (2, 2, "A"))
GROUPS = (((0, 1), (4,)), ((2, 3), (3,)), ((4, 5), (2,)), ((6, 7), (1, 0)))
RPOS = (15, 16, 0, 1, 2, 17, 3, 4, 5, 18, 6, 7, 8, 9, 10, 11, 12, 13, 14)
KZ = (3, 4, 0, 1, 2)
KP = (6, 0, 1, 2)
KN = (7, 3, 4, 5)


def geometry(gx, gy, gz, div, rem):
    y, xh, xl, c = div(gx, 2), rem(gx, 2), div(gy, 2), rem(gy, 2)
    xor = lambda a, b: a + b - 2 * a * b
    dev = dict(
        right=(y * 2 + xor(xh, xl), 2 * (1 - xl) + c, gz),
        left=(y * 2 + xor(xh, 1 - xl), 2 * (1 - xl) + c, gz),
        yt=(rem(y + 5 - 2 * xh, 4) * 2 + xh, gy, gz),
        ys=(rem(y + 3 + 2 * xh, 4) * 2 + xh, gy, gz),
        zp=(gx, gy, rem(gz + 1, 8)),
        zm=(gx, gy, rem(gz + 7, 8)),
        partner=(gx, 2 * xl + 1 - c, gz),
    )
    dev["relay"] = tuple(a * (1 - c) + b * c for a, b in zip(dev["right"], dev["left"]))
    s, t = 1 - 2 * xh, 1 - 2 * c
    blocks = []
    for q in range(27):
        if q < 9:
            da, db = (0, s, -s)[q // 3], 0
        else:
            p = (q - 9) // 3
            da = (0, s, -s, (1 - xl) * s, xl * s, -s)[p]
            db = (t, t, t, -t, -t, -t)[p]
        blocks.append((da + 1) * 9 + (db + 1) * 3 + q % 3)
    return dev, c, xl, blocks


def chunk_ops(k, route):
    ops = []
    S, O, YO, L, R, YC = (3 * p for p in range(6))
    dks = (1, 0, 2) if route == "A" else (1,)
    if route == "A":
        ops.append((k, "zp", S + 1, S + 0, ()))
        ops.append((k, "zm", S + 1, S + 2, ()))
    for d in dks:
        pre = () if d == 1 else ((k, S + d),)
        ops.append((k, "right", S + d, L + d, pre))
        ops.append((k, "left", S + d, R + d, pre))
    for d in dks:
        ops.append((k, "relay", "F%d" % d, O + d, ((k, L + d), (k, R + d))))
    for d in dks:
        ops.append((k, "yt", "C%d" % d, YC + d, ((k, L + d), (k, R + d))))
        ops.append((k, "yt", O + d, YO + d, ((k, O + d),)))
    if route == "B":
        for p in range(6):
            pre = () if p == 0 else ((k, 3 * p + 1),)
            ops.append((k, "zp", 3 * p + 1, 3 * p + 0, pre))
            ops.append((k, "zm", 3 * p + 1, 3 * p + 2, pre))
    for p in range(6):
        pre = tuple((k, 3 * p + d) for d in range(3) if not (p == 0 and d == 1))
        ops.append((k, "partner", 3 * p, 100 + 3 * p, pre))
    return ops


def plan(pieces, lat=2.7, rate=46.6e3):
    ops = [op for k, (_, _, r) in enumerate(CHUNKS) for op in chunk_ops(k, r)]
    pend, free, arrive, seq, now = list(ops), {}, {}, [], 0.0
    pieces = list(pieces)

    def group_ready(g):
        if g < 0:
            return 0.0
        keys = [(k, 100 + 3 * p) for k in GROUPS[g][0] for p in range(6)]
        return max(arrive.get(key, 1e9) for key in keys)

    while pend or pieces:
        ready = [op for op in pend if all(arrive.get(x, 1e9) <= now for x in op[4])]
        if ready:
            op = ready[0]
            pend.remove(op)
            seq.append(("op", op))
            k, link, _, dst, _ = op
            size = 32 * CHUNKS[k][1] * 256 * (3 if link == "partner" else 1)
            lk = "right" if link == "relay" else link
            r = 300e3 if link == "partner" else rate * (1.33 if lk == "right" else 1.0)
            start = max(now, free.get(lk, 0.0))
            free[lk] = start + size / r
            arrive[(k, dst)] = free[lk] + (1.0 if link == "partner" else lat)
            now += 0.02
            continue
        if pieces and group_ready(pieces[0][2]) <= now:
            name, us, _ = pieces.pop(0)
            seq.append(("piece", name))
            now += us
            continue
        times = [max([arrive.get(x, 1e9) for x in op[4]]) for op in pend]
        if pieces:
            times.append(group_ready(pieces[0][2]))
        now = max(now, min(times))
    return seq, now, arrive

EPS = 1e-06
NK = len(CHUNKS)


def make_pieces():
    pieces = [("own", 0.7, -1), ("onehot", 0.4, -1)]
    pieces += [("frames%d" % g, 0.15, -1) for g in range(4)]
    pieces += [("weights%d" % i, 0.3, -1) for i in range(10)]
    for gi, (_, degrees) in enumerate(GROUPS):
        lo, hi = degrees[-1] ** 2, (degrees[0] + 1) ** 2
        last = gi == len(GROUPS) - 1
        step = hi - lo if last else 2
        if last:
            pieces += [("early%d" % i, 0.3, -1) for i in range(8)]
        j = lo
        while j < hi:
            n = min(step, hi - j)
            pieces.append(("gather%d:%d:%d:%d" % (gi, j, n, lo), 0.22 * n, gi))
            j += n
        for l in degrees:
            for e in range(4):
                pieces.append(("rotate%d:%d:%d" % (l, e, lo), 0.005 * (2 * l + 1) * min(5, 2 * l + 1), gi))
    return pieces


def rotate_tile(l, e, base, gl, wb, rot):
    d = 2 * l + 1
    e0 = e * 128
    for c in range(0, CH, 16):
        g = [[gl[(base + j) * CH + c + 8 * h:(base + j) * CH + c + 8 * h + 8, e0:e0 + 128] for h in range(2)] for j in range(d)]
        for pos, ps in ROWS[l]:
            acc = [None, None]
            for j in range(d):
                f = wb[SLOT[ps[j]], :, e0:e0 + 128]
                for h in range(2):
                    t = f * g[j][h]
                    acc[h] = t if acc[h] is None else acc[h] + t
            r = RPOS[pos] * CH + c
            rot[r:r + 16, e0:e0 + 128] = jnp.concatenate(acc, axis=0).astype(BF16)


def weight_blocks():
    todo = []
    for v in range(2):
        todo += [(v, 0, a, b) for a in range(5) for b in range(5)]
        todo += [(v, 1, a, b) for a in range(4) for b in range(4)]
        todo += [(v, 2, a, b) for a in range(3) for b in range(3)]
    return todo


def build_block(v, m, a, b, raw, built):
    src, dst, n = raw[m], built[m], (5, 4, 3)[m]
    blk = lambda i: slice(i * CH, (i + 1) * CH)
    if m == 0:
        dst[v, blk(b), blk(a if v else KZ[a])] = src[v, blk(a), blk(b)].T
        return
    p, q = (KP[a], KN[a]) if m == 1 and v == 0 else (a, n + a)
    re, im = src[v, 0, blk(a), blk(b)].T, src[v, 1, blk(a), blk(b)].T
    dst[v, blk(b), blk(p)] = re
    dst[v, blk(n + b), blk(q)] = re
    dst[v, blk(b), blk(q)] = -im
    dst[v, blk(n + b), blk(p)] = im


def early_conv(i, rot, wzt, w1t, w2t, hid):
    if i == 0:
        hid[0:640, :] = dot(wzt[0, :, 0:384], rot[0:384, :])
    elif i < 5:
        b = i - 1
        hid[640 + b * 256:896 + b * 256, :] = dot(w1t[0, b * 256:(b + 1) * 256, 0:768], rot[384:1152, :])
    else:
        b = i - 5
        hid[1664 + b * 256:1920 + b * 256, :] = dot(w2t[0, b * 256:(b + 1) * 256, :], rot[1152:1920, :])


def merged_kernel(cnt, blocks, src_h, tgt_h, halo_h, attn_h, coeffs, wig_h, wz_h, w1_h, w2_h, out,
                  src, tgt, halo, attn, cf, wig, wzr, w1r, w2r, tab, tabo, tabt, wb, wzt, w1t, w2t,
                  oh, gl, rot, act, wei, msg, attb, sigs, hid, lsem, ssem, rsem):
    MESH = pl.DeviceIdType.MESH
    gx, gy, gz = (lax.axis_index(n) for n in ("gx", "gy", "gz"))
    dev, core, xl, bids = geometry(gx, gy, gz, lax.div, lax.rem)

    loads = [pltpu.make_async_copy(a, b, lsem.at[i]) for i, (a, b) in enumerate(
        ((halo_h.at[0, 0], halo), (coeffs.at[0, 0, 0], cf), (src_h.at[0, 0, 0], src), (tgt_h.at[0, 0, 0], tgt), (attn_h, attn),
         (wig_h.at[0, 0, 0], wig), (wz_h, wzr), (w1_h, w1r), (w2_h, w2r)))]
    for cp in loads:
        cp.start()
    barrier = pltpu.get_barrier_semaphore()
    near = ("right", "left", "yt", "ys", "zp", "zm", "partner")
    for n in near:
        pl.semaphore_signal(barrier, inc=1, device_id=dev[n], device_id_type=MESH)

    loads[0].wait()
    pick = jnp.where(lax.broadcasted_iota(jnp.int32, (128, 32), 0) == halo[...], 1.0, 0.0).astype(F32).T.astype(BF16)
    loads[1].wait()
    rows = dot(pick, cf[...])
    rows = rows * lax.rsqrt(jnp.mean(rows * rows, axis=-1, keepdims=True) + EPS)
    tab[32:64, :] = rows.astype(BF16)
    tab[864:896, :] = jnp.zeros((32, 3200), BF16)
    pl.semaphore_wait(barrier, len(near))

    descs = {}

    def issue(op):
        k, link, s, d, _ = op
        j0, n, _ = CHUNKS[k]
        cols = pl.ds(j0 * CH, n * CH)
        cnt_slots = 3 if link == "partner" else 1
        if isinstance(s, str):
            sel = core if s[0] == "F" else xl
            row = pl.multiple_of((3 * sel + int(s[1])) * 32, 32)
            sref = tabo.at[pl.ds(row, 32), cols]
        elif s < 9:
            sref = tab.at[pl.ds(32 * s, 32 * cnt_slots), cols]
        else:
            sref = tabo.at[pl.ds(32 * (s - 9), 32 * cnt_slots), cols]
        if d >= 100:
            dref = tab.at[pl.ds(288 + 32 * (d - 100), 96), cols]
        elif d < 9:
            dref = tab.at[pl.ds(32 * d, 32), cols]
        else:
            dref = tabo.at[pl.ds(32 * (d - 9), 32), cols]
        i = len(descs)
        cp = pltpu.make_async_remote_copy(src_ref=sref, dst_ref=dref, send_sem=ssem.at[i], recv_sem=rsem.at[i],
                                          device_id=dev[link], device_id_type=MESH)
        descs[(k, d)] = cp
        return cp

    waited = set()

    def arrive(key):
        if key not in waited:
            waited.add(key)
            descs[key].wait_recv()

    raw, built = (wzr, w1r, w2r), (wzt, w1t, w2t)
    wblocks = weight_blocks()

    def piece(name):
        if name == "own":
            x = cf[...].astype(F32)
            f = lax.rsqrt(jnp.mean(x * x, axis=-1, keepdims=True) + EPS)
            for j in range(25):
                tabt[j * CH:(j + 1) * CH, 0:128] = (cf[:, j * CH:(j + 1) * CH].astype(F32) * f).astype(BF16).T
        elif name == "onehot":
            for cp in loads[2:5]:
                cp.wait()
            own = lax.broadcasted_iota(jnp.int32, (128, 128), 0)
            for g in range(4):
                oh[0:128, g * 128:(g + 1) * 128] = jnp.where(own == src[g:g + 1, :], 1.0, 0.0).astype(BF16)
                for q in range(27):
                    at = lax.broadcasted_iota(jnp.int32, (32, 128), 0) + (128 + 32 * bids[q])
                    oh[128 + 32 * q:160 + 32 * q, g * 128:(g + 1) * 128] = jnp.where(at == src[g:g + 1, :], 1.0, 0.0).astype(BF16)
                oh[992:1024, g * 128:(g + 1) * 128] = jnp.zeros((32, 128), BF16)
        elif name.startswith("frames"):
            g = int(name[6:])
            if g == 0:
                loads[5].wait()
            for i, p in enumerate(USED):
                wb[i, :, g * 128:(g + 1) * 128] = jnp.broadcast_to(wig[p, g:g + 1, :].astype(F32), (8, 128))
        elif name.startswith("weights"):
            i = int(name[7:])
            if i == 0:
                for cp in loads[6:]:
                    cp.wait()
            for blk in wblocks[i * 10:(i + 1) * 10]:
                build_block(*blk, raw, built)
        elif name.startswith("gather"):
            gi, j0, n, lo = (int(v) for v in name[6:].split(":"))
            for j in range(j0, j0 + n):
                for g in range(7):
                    tabt[j * CH:(j + 1) * CH, 128 + g * 128:256 + g * 128] = tab[g * 128:(g + 1) * 128, j * CH:(j + 1) * CH].T
            gl[(j0 - lo) * CH:(j0 - lo + n) * CH, :] = dot(tabt[j0 * CH:(j0 + n) * CH, :], oh[...])
        elif name.startswith("rotate"):
            l, e, lo = (int(v) for v in name[6:].split(":"))
            rotate_tile(l, e, l * l - lo, gl, wb, rot)
        elif name.startswith("early"):
            early_conv(int(name[5:]), rot, wzt, w1t, w2t, hid)

    got = set()
    seq, _, _ = plan(make_pieces())
    for kind, what in seq:
        if kind == "op":
            for key in what[4]:
                arrive(key)
            issue(what).start()
        else:
            if what[:6] == "gather":
                g = int(what[6:].split(":")[0])
                if g not in got:
                    got.add(g)
                    for k in GROUPS[g][0]:
                        for p in range(6):
                            arrive((k, 100 + 3 * p))
            piece(what)
    for key, cp in descs.items():
        arrive(key)
        cp.wait_send()

    finish(tgt, cnt, blocks, attn, wb, wzt, w1t, w2t, out, oh, rot, act, wei, msg, attb, sigs, hid)


def finish(tgt, cnt, blocks, attn_ref, wb, wzt, w1t, w2t, out, oh, rot, act, wei, msg, attb, sigs, hid):
    attn = jnp.broadcast_to(attn_ref[...], (128, 128)).T

    def emit1(c0, n, val):
        if c0 == 0:
            sig = jax.nn.sigmoid(val)
            sigs[...] = sig
            silu = val * sig
            act[0:128, :] = silu.astype(BF16)
            for g in range(4):
                t = (silu[:, g * 128:(g + 1) * 128] * attn).reshape(8, 16, 128)
                logit = jnp.sum(t, axis=1)
                edge = lax.broadcasted_iota(jnp.int32, (8, 128), 1)
                live = jnp.logical_and(edge < cnt[0, 0, 0, g], g < blocks[0, 0, 0])
                a = jnp.where(live, jax.nn.sigmoid(logit), 0.0)
                attb[:, g * 128:(g + 1) * 128] = jnp.broadcast_to(a[:, None, :], (8, 16, 128)).reshape(128, 128)
        else:
            for k in range(n):
                act[(c0 + k) * CH:(c0 + k + 1) * CH, :] = (val[k * CH:(k + 1) * CH] * sigs[...]).astype(BF16)
    z = rot[15 * CH:17 * CH, :]
    for c0, n in ((0, 1), (1, 2), (3, 2)):
        emit1(c0, n, hid[c0 * CH:(c0 + n) * CH, :] + dot(wzt[0, c0 * CH:(c0 + n) * CH, 384:640], z))
    one = rot[17 * CH:19 * CH, :]
    for b in range(4):
        emit1(5 + 2 * b, 2, hid[640 + b * 256:896 + b * 256, :] + dot(w1t[0, b * 256:(b + 1) * 256, 768:1024], one))
    for b in range(3):
        emit1(13 + 2 * b, 2, hid[1664 + b * 256:1920 + b * 256, :])

    def emit2(c0, n, val):
        for k in range(n):
            wei[(c0 + k) * CH:(c0 + k + 1) * CH, :] = (val[k * CH:(k + 1) * CH] * attb[...]).astype(BF16)
    conv_parts(1, act, wzt, w1t, w2t, emit2)

    for g in range(4):
        atom = lax.broadcasted_iota(jnp.int32, (128, 128), 0)
        oh[0:128, g * 128:(g + 1) * 128] = jnp.where(atom == tgt[g:g + 1, :], 1.0, 0.0).astype(BF16)
    for l in range(5):
        rotate_out(l, wei, wb, msg)
        lo, hi = l * l * CH, (l + 1) * (l + 1) * CH
        upd = lax.dot_general(oh[0:128, :], msg[lo:hi, :], (((1,), (1,)), ((), ())), preferred_element_type=F32)
        out[0, 0, 0, :, lo:hi] = upd.astype(BF16)


def body(coeffs, halo_rows, edge_source, edge_target, edge_count, block_count, wigner, w_zero, w_one, w_two, attn_vector):
    vm = pl.BlockSpec(memory_space=pltpu.VMEM)
    sm = pl.BlockSpec(memory_space=pltpu.SMEM)
    hb = pl.BlockSpec(memory_space=pl.ANY)
    nops = sum(len(chunk_ops(k, r)) for k, (_, _, r) in enumerate(CHUNKS))
    V = pltpu.VMEM
    return pl.pallas_call(
        merged_kernel,
        out_shape=jax.ShapeDtypeStruct((1, 1, 1, 128, 3200), BF16),
        in_specs=[sm, sm] + [hb] * 9,
        out_specs=vm,
        scratch_shapes=[
            V((4, 128), jnp.int32), V((4, 128), jnp.int32), V((1, 32), jnp.int32), V((1, 128), F32), V((128, 3200), BF16), V((165, 4, 128), BF16), V((2, 640, 640), BF16), V((2, 2, 512, 512), BF16), V((2, 2, 384, 384), BF16),
            V((896, 3200), BF16), V((288, 3200), BF16), V((3200, 1024), BF16), V((115, 8, NE), F32),
            V((2, 640, 640), BF16), V((2, 1024, 1024), BF16), V((2, 768, 768), BF16),
            V((1024, NE), BF16), V((9 * CH, NE), F32), V((19 * CH, NE), BF16), V((19 * CH, NE), BF16), V((19 * CH, NE), BF16),
            V((25 * CH, NE), BF16), V((CH, NE), F32), V((CH, NE), F32), V((19 * CH, NE), F32),
            pltpu.SemaphoreType.DMA((9,)), pltpu.SemaphoreType.DMA((nops,)), pltpu.SemaphoreType.DMA((nops,)),
        ],
        compiler_params=pltpu.CompilerParams(vmem_limit_bytes=67043328, collective_id=0, has_side_effects=True),
    )(edge_count, block_count, edge_source, edge_target, halo_rows, attn_vector.reshape(1, 128), coeffs, jnp.transpose(wigner, (0, 1, 2, 4, 3, 5)), w_zero, w_one, w_two)


def solution(mesh):
    placed = (P("gx", "gy", "gz", None, None), P("gx", "gy", "gz", None), P("gx", "gy", "gz", None, None), P("gx", "gy", "gz", None, None),
              P("gx", "gy", "gz", None), P("gx", "gy", "gz"), P("gx", "gy", "gz", None, None, None), P(), P(), P(), P())
    return jax.shard_map(body, mesh=mesh, in_specs=placed, out_specs=P("gx", "gy", "gz", None, None), check_vma=False)
```

```python
import math
import functools
import jax, jax.numpy as jnp, numpy as np
from jax import lax
from jax.experimental import pallas as pl
from jax.experimental.pallas import tpu as pltpu
from jax.sharding import PartitionSpec as P

CH = 128
F32 = jnp.float32
BF16 = jnp.bfloat16
STARTS = [0, 1, 10, 35, 84]
ORDER = [0, 2, 6, 12, 20, 3, 7, 13, 21, 1, 5, 11, 19, 8, 14, 22, 4, 10, 18]
ROWS = []
for l in range(5):
    rows = []
    for pos, comp in enumerate(ORDER):
        if math.isqrt(comp) == l:
            off = comp - l * l
            rows.append((pos, [STARTS[l] + off * (2 * l + 1) + j for j in range(2 * l + 1)]))
    ROWS.append(rows)
USED = sorted({p for rows in ROWS for _, ps in rows for p in ps})
SLOT = {p: i for i, p in enumerate(USED)}
NE = 512


def rotate_out(l, wei, wb, msg):
    d = 2 * l + 1
    for e in range(0, NE, 128):
        for c in range(0, CH, 16):
            w = [wei[pos * CH + c:pos * CH + c + 16, e:e + 128].astype(F32) for pos, _ in ROWS[l]]
            for j in range(d):
                acc = [None, None]
                for n, (pos, ps) in enumerate(ROWS[l]):
                    f = wb[SLOT[ps[j]], :, e:e + 128]
                    for h in range(2):
                        t = f * w[n][8 * h:8 * h + 8]
                        acc[h] = t if acc[h] is None else acc[h] + t
                r = (l * l + j) * CH + c
                msg[r:r + 16, e:e + 128] = jnp.concatenate(acc, axis=0).astype(BF16)


def dot(a, b):
    return jnp.dot(a, b, preferred_element_type=F32)


def conv_parts(v, x, wzt, w1t, w2t, emit):
    emit(0, 1, dot(wzt[v, 0:128, :], x[0:640, :]))
    emit(1, 2, dot(wzt[v, 128:384, :], x[0:640, :]))
    emit(3, 2, dot(wzt[v, 384:640, :], x[0:640, :]))
    for b in range(4):
        emit(5 + 2 * b, 2, dot(w1t[v, b * 256:(b + 1) * 256, :], x[640:1664, :]))
    for b in range(3):
        emit(13 + 2 * b, 2, dot(w2t[v, b * 256:(b + 1) * 256, :], x[1664:2432, :]))


P_S, P_O, P_YO, P_L, P_R, P_YC = range(6)
LINKS = ("right", "left", "yt", "zp", "zm", "partner")
CHUNKS = ((16, 6, 'B'), (22, 3, 'A'), (9, 3, 'B'), (12, 4, 'B'), (4, 5, 'A'), (0, 4, 'B'))
GROUPS = (((0, 1), (4,)), ((2, 3), (3,)), ((4,), (2,)), ((5,), (1, 0)))
RPOS = (15, 16, 0, 1, 2, 17, 3, 4, 5, 18, 6, 7, 8, 9, 10, 11, 12, 13, 14)
KZ = (3, 4, 0, 1, 2)
KP = (6, 0, 1, 2)
KN = (7, 3, 4, 5)


def geometry(gx, gy, gz, div, rem):
    y, xh, xl, c = div(gx, 2), rem(gx, 2), div(gy, 2), rem(gy, 2)
    xor = lambda a, b: a + b - 2 * a * b
    dev = dict(
        right=(y * 2 + xor(xh, xl), 2 * (1 - xl) + c, gz),
        left=(y * 2 + xor(xh, 1 - xl), 2 * (1 - xl) + c, gz),
        yt=(rem(y + 5 - 2 * xh, 4) * 2 + xh, gy, gz),
        ys=(rem(y + 3 + 2 * xh, 4) * 2 + xh, gy, gz),
        zp=(gx, gy, rem(gz + 1, 8)),
        zm=(gx, gy, rem(gz + 7, 8)),
        partner=(gx, 2 * xl + 1 - c, gz),
    )
    dev["relay"] = tuple(a * (1 - c) + b * c for a, b in zip(dev["right"], dev["left"]))
    s, t = 1 - 2 * xh, 1 - 2 * c
    blocks = []
    for q in range(27):
        if q < 9:
            da, db = (0, s, -s)[q // 3], 0
        else:
            p = (q - 9) // 3
            da = (0, s, -s, (1 - xl) * s, xl * s, -s)[p]
            db = (t, t, t, -t, -t, -t)[p]
        blocks.append((da + 1) * 9 + (db + 1) * 3 + q % 3)
    return dev, c, xl, blocks


def chunk_ops(k, route):
    ops = []
    S, O, YO, L, R, YC = (3 * p for p in range(6))
    dks = (1, 0, 2) if route == "A" else (1,)
    if route == "A":
        ops.append((k, "zp", S + 1, S + 0, ()))
        ops.append((k, "zm", S + 1, S + 2, ()))
    for d in dks:
        pre = () if d == 1 else ((k, S + d),)
        ops.append((k, "right", S + d, L + d, pre))
        ops.append((k, "left", S + d, R + d, pre))
    for d in dks:
        ops.append((k, "relay", "F%d" % d, O + d, ((k, L + d), (k, R + d))))
    for d in dks:
        ops.append((k, "yt", "C%d" % d, YC + d, ((k, L + d), (k, R + d))))
        ops.append((k, "yt", O + d, YO + d, ((k, O + d),)))
    if route == "B":
        for p in range(6):
            pre = () if p == 0 else ((k, 3 * p + 1),)
            ops.append((k, "zp", 3 * p + 1, 3 * p + 0, pre))
            ops.append((k, "zm", 3 * p + 1, 3 * p + 2, pre))
    for p in range(6):
        pre = tuple((k, 3 * p + d) for d in range(3) if not (p == 0 and d == 1))
        ops.append((k, "partner", 3 * p, 100 + 3 * p, pre))
    return ops


def plan(pieces, lat=2.4, rate=46.6e3, window=0.3):
    ops = [op for k, (_, _, r) in enumerate(CHUNKS) for op in chunk_ops(k, r)]
    group_of = {k: g for g, (ks, _) in enumerate(GROUPS) for k in ks}
    pend = sorted(ops, key=lambda op: group_of[op[0]])
    free, arrive, seq, now = {}, {}, [], 0.0
    pieces = list(pieces)

    def group_ready(g):
        if g < 0:
            return 0.0
        keys = [(k, 100 + 3 * p) for k in GROUPS[g][0] for p in range(6)]
        return max(arrive.get(key, 1e9) for key in keys)

    def link(op):
        return "right" if op[1] == "relay" else op[1]

    while pend or pieces:
        open_at = [max([arrive.get(x, 1e9) for x in op[4]] + [free.get(link(op), 0.0) - window]) for op in pend]
        ready = [op for op, t in zip(pend, open_at) if t <= now]
        if ready:
            op = ready[0]
            pend.remove(op)
            seq.append(("op", op))
            k, name, _, dst, _ = op
            size = 32 * CHUNKS[k][1] * 256 * (3 if name == "partner" else 1)
            r = 300e3 if name == "partner" else rate * (1.33 if link(op) == "right" else 1.0)
            start = max(now, free.get(link(op), 0.0))
            free[link(op)] = start + size / r
            arrive[(k, dst)] = free[link(op)] + (1.0 if name == "partner" else lat)
            now += 0.02
            continue
        if pieces and group_ready(pieces[0][2]) <= now:
            name, us, _ = pieces.pop(0)
            seq.append(("piece", name))
            now += us
            continue
        now = max(now, min(open_at + [group_ready(p[2]) for p in pieces[:1]]))
    return seq, now, arrive


EPS = 1e-06
NK = len(CHUNKS)


def make_pieces():
    pieces = [("own", 0.7, -1), ("onehot", 0.4, -1)]
    pieces += [("frames%d" % g, 0.15, -1) for g in range(4)]
    pieces += [("weights%d" % i, 0.3, -1) for i in range(10)]
    for gi, (_, degrees) in enumerate(GROUPS):
        lo, hi = degrees[-1] ** 2, (degrees[0] + 1) ** 2
        last = gi == len(GROUPS) - 1
        step = hi - lo if last else 2
        if last:
            pieces += [("early%d" % i, 0.3, -1) for i in range(8)]
        j = lo
        while j < hi:
            n = min(step, hi - j)
            pieces.append(("gather%d:%d:%d:%d" % (gi, j, n, lo), 0.22 * n, gi))
            j += n
        for l in degrees:
            for e in range(4):
                pieces.append(("rotate%d:%d:%d" % (l, e, lo), 0.005 * (2 * l + 1) * min(5, 2 * l + 1), gi))
    return pieces


def rotate_tile(l, e, base, gl, wb, rot):
    d = 2 * l + 1
    e0 = e * 128
    for c in range(0, CH, 16):
        g = [[gl[(base + j) * CH + c + 8 * h:(base + j) * CH + c + 8 * h + 8, e0:e0 + 128] for h in range(2)] for j in range(d)]
        for pos, ps in ROWS[l]:
            acc = [None, None]
            for j in range(d):
                f = wb[SLOT[ps[j]], :, e0:e0 + 128]
                for h in range(2):
                    t = f * g[j][h]
                    acc[h] = t if acc[h] is None else acc[h] + t
            r = RPOS[pos] * CH + c
            rot[r:r + 16, e0:e0 + 128] = jnp.concatenate(acc, axis=0).astype(BF16)


def weight_blocks():
    todo = []
    for v in range(2):
        todo += [(v, 0, a, b) for a in range(5) for b in range(5)]
        todo += [(v, 1, a, b) for a in range(4) for b in range(4)]
        todo += [(v, 2, a, b) for a in range(3) for b in range(3)]
    return todo


def build_block(v, m, a, b, raw, built):
    src, dst, n = raw[m], built[m], (5, 4, 3)[m]
    blk = lambda i: slice(i * CH, (i + 1) * CH)
    if m == 0:
        dst[v, blk(b), blk(a if v else KZ[a])] = src[v, blk(a), blk(b)].T
        return
    p, q = (KP[a], KN[a]) if m == 1 and v == 0 else (a, n + a)
    re, im = src[v, 0, blk(a), blk(b)].T, src[v, 1, blk(a), blk(b)].T
    dst[v, blk(b), blk(p)] = re
    dst[v, blk(n + b), blk(q)] = re
    dst[v, blk(b), blk(q)] = -im
    dst[v, blk(n + b), blk(p)] = im


def early_conv(i, rot, wzt, w1t, w2t, hid):
    if i == 0:
        hid[0:640, :] = dot(wzt[0, :, 0:384], rot[0:384, :])
    elif i < 5:
        b = i - 1
        hid[640 + b * 256:896 + b * 256, :] = dot(w1t[0, b * 256:(b + 1) * 256, 0:768], rot[384:1152, :])
    else:
        b = i - 5
        hid[1664 + b * 256:1920 + b * 256, :] = dot(w2t[0, b * 256:(b + 1) * 256, :], rot[1152:1920, :])


def merged_kernel(cnt, blocks, src_h, tgt_h, halo_h, attn_h, coeffs, wig_h, wz_h, w1_h, w2_h, out,
                  src, tgt, halo, attn, cf, wig, wzr, w1r, w2r, tab, tabo, tabt, wb, wzt, w1t, w2t,
                  oh, gl, rot, act, wei, msg, attb, sigs, hid, lsem, ssem, rsem):
    MESH = pl.DeviceIdType.MESH
    gx, gy, gz = (lax.axis_index(n) for n in ("gx", "gy", "gz"))
    dev, core, xl, bids = geometry(gx, gy, gz, lax.div, lax.rem)

    loads = [pltpu.make_async_copy(a, b, lsem.at[i]) for i, (a, b) in enumerate(
        ((halo_h.at[0, 0], halo), (coeffs.at[0, 0, 0], cf), (src_h.at[0, 0, 0], src), (tgt_h.at[0, 0, 0], tgt), (attn_h, attn),
         (wig_h.at[0, 0, 0], wig), (wz_h, wzr), (w1_h, w1r), (w2_h, w2r)))]
    for cp in loads:
        cp.start()
    barrier = pltpu.get_barrier_semaphore()
    near = ("right", "left", "yt", "ys", "zp", "zm", "partner")
    for n in near:
        pl.semaphore_signal(barrier, inc=1, device_id=dev[n], device_id_type=MESH)

    loads[0].wait()
    pick = jnp.where(lax.broadcasted_iota(jnp.int32, (128, 32), 0) == halo[...], 1.0, 0.0).astype(F32).T.astype(BF16)
    loads[1].wait()
    rows = dot(pick, cf[...])
    rows = rows * lax.rsqrt(jnp.mean(rows * rows, axis=-1, keepdims=True) + EPS)
    tab[32:64, :] = rows.astype(BF16)
    tab[864:896, :] = jnp.zeros((32, 3200), BF16)
    pl.semaphore_wait(barrier, len(near))

    descs = {}

    def issue(op):
        k, link, s, d, _ = op
        j0, n, _ = CHUNKS[k]
        cols = pl.ds(j0 * CH, n * CH)
        cnt_slots = 3 if link == "partner" else 1
        if isinstance(s, str):
            sel = core if s[0] == "F" else xl
            row = pl.multiple_of((3 * sel + int(s[1])) * 32, 32)
            sref = tabo.at[pl.ds(row, 32), cols]
        elif s < 9:
            sref = tab.at[pl.ds(32 * s, 32 * cnt_slots), cols]
        else:
            sref = tabo.at[pl.ds(32 * (s - 9), 32 * cnt_slots), cols]
        if d >= 100:
            dref = tab.at[pl.ds(288 + 32 * (d - 100), 96), cols]
        elif d < 9:
            dref = tab.at[pl.ds(32 * d, 32), cols]
        else:
            dref = tabo.at[pl.ds(32 * (d - 9), 32), cols]
        i = len(descs)
        cp = pltpu.make_async_remote_copy(src_ref=sref, dst_ref=dref, send_sem=ssem.at[i], recv_sem=rsem.at[i],
                                          device_id=dev[link], device_id_type=MESH)
        descs[(k, d)] = cp
        return cp

    waited = set()

    def arrive(key):
        if key not in waited:
            waited.add(key)
            descs[key].wait_recv()

    raw, built = (wzr, w1r, w2r), (wzt, w1t, w2t)
    wblocks = weight_blocks()

    def piece(name):
        if name == "own":
            x = cf[...].astype(F32)
            f = lax.rsqrt(jnp.mean(x * x, axis=-1, keepdims=True) + EPS)
            for j in range(25):
                tabt[j * CH:(j + 1) * CH, 0:128] = (cf[:, j * CH:(j + 1) * CH].astype(F32) * f).astype(BF16).T
        elif name == "onehot":
            for cp in loads[2:5]:
                cp.wait()
            own = lax.broadcasted_iota(jnp.int32, (128, 128), 0)
            for g in range(4):
                oh[0:128, g * 128:(g + 1) * 128] = jnp.where(own == src[g:g + 1, :], 1.0, 0.0).astype(BF16)
                for q in range(27):
                    at = lax.broadcasted_iota(jnp.int32, (32, 128), 0) + (128 + 32 * bids[q])
                    oh[128 + 32 * q:160 + 32 * q, g * 128:(g + 1) * 128] = jnp.where(at == src[g:g + 1, :], 1.0, 0.0).astype(BF16)
                oh[992:1024, g * 128:(g + 1) * 128] = jnp.zeros((32, 128), BF16)
        elif name.startswith("frames"):
            g = int(name[6:])
            if g == 0:
                loads[5].wait()
            for i, p in enumerate(USED):
                wb[i, :, g * 128:(g + 1) * 128] = jnp.broadcast_to(wig[p, g:g + 1, :].astype(F32), (8, 128))
        elif name.startswith("weights"):
            i = int(name[7:])
            if i == 0:
                for cp in loads[6:]:
                    cp.wait()
            for blk in wblocks[i * 10:(i + 1) * 10]:
                build_block(*blk, raw, built)
        elif name.startswith("gather"):
            gi, j0, n, lo = (int(v) for v in name[6:].split(":"))
            for j in range(j0, j0 + n):
                for g in range(7):
                    tabt[j * CH:(j + 1) * CH, 128 + g * 128:256 + g * 128] = tab[g * 128:(g + 1) * 128, j * CH:(j + 1) * CH].T
            gl[(j0 - lo) * CH:(j0 - lo + n) * CH, :] = dot(tabt[j0 * CH:(j0 + n) * CH, :], oh[...])
        elif name.startswith("rotate"):
            l, e, lo = (int(v) for v in name[6:].split(":"))
            rotate_tile(l, e, l * l - lo, gl, wb, rot)
        elif name.startswith("early"):
            early_conv(int(name[5:]), rot, wzt, w1t, w2t, hid)

    got = set()
    seq, _, _ = plan(make_pieces())
    for kind, what in seq:
        if kind == "op":
            for key in what[4]:
                arrive(key)
            issue(what).start()
        else:
            if what[:6] == "gather":
                g = int(what[6:].split(":")[0])
                if g not in got:
                    got.add(g)
                    for k in GROUPS[g][0]:
                        for p in range(6):
                            arrive((k, 100 + 3 * p))
            piece(what)
    for key, cp in descs.items():
        arrive(key)
        cp.wait_send()

    finish(tgt, cnt, blocks, attn, wb, wzt, w1t, w2t, out, oh, rot, act, wei, msg, attb, sigs, hid)


def finish(tgt, cnt, blocks, attn_ref, wb, wzt, w1t, w2t, out, oh, rot, act, wei, msg, attb, sigs, hid):
    attn = jnp.broadcast_to(attn_ref[...], (128, 128)).T

    def emit1(c0, n, val):
        if c0 == 0:
            sig = jax.nn.sigmoid(val)
            sigs[...] = sig
            silu = val * sig
            act[0:128, :] = silu.astype(BF16)
            for g in range(4):
                t = (silu[:, g * 128:(g + 1) * 128] * attn).reshape(8, 16, 128)
                logit = jnp.sum(t, axis=1)
                edge = lax.broadcasted_iota(jnp.int32, (8, 128), 1)
                live = jnp.logical_and(edge < cnt[0, 0, 0, g], g < blocks[0, 0, 0])
                a = jnp.where(live, jax.nn.sigmoid(logit), 0.0)
                attb[:, g * 128:(g + 1) * 128] = jnp.broadcast_to(a[:, None, :], (8, 16, 128)).reshape(128, 128)
        else:
            for k in range(n):
                act[(c0 + k) * CH:(c0 + k + 1) * CH, :] = (val[k * CH:(k + 1) * CH] * sigs[...]).astype(BF16)
    z = rot[15 * CH:17 * CH, :]
    for c0, n in ((0, 1), (1, 2), (3, 2)):
        emit1(c0, n, hid[c0 * CH:(c0 + n) * CH, :] + dot(wzt[0, c0 * CH:(c0 + n) * CH, 384:640], z))
    one = rot[17 * CH:19 * CH, :]
    for b in range(4):
        emit1(5 + 2 * b, 2, hid[640 + b * 256:896 + b * 256, :] + dot(w1t[0, b * 256:(b + 1) * 256, 768:1024], one))
    for b in range(3):
        emit1(13 + 2 * b, 2, hid[1664 + b * 256:1920 + b * 256, :])

    def emit2(c0, n, val):
        for k in range(n):
            wei[(c0 + k) * CH:(c0 + k + 1) * CH, :] = (val[k * CH:(k + 1) * CH] * attb[...]).astype(BF16)
    conv_parts(1, act, wzt, w1t, w2t, emit2)

    for g in range(4):
        atom = lax.broadcasted_iota(jnp.int32, (128, 128), 0)
        oh[0:128, g * 128:(g + 1) * 128] = jnp.where(atom == tgt[g:g + 1, :], 1.0, 0.0).astype(BF16)
    for l in range(5):
        rotate_out(l, wei, wb, msg)
        lo, hi = l * l * CH, (l + 1) * (l + 1) * CH
        upd = lax.dot_general(oh[0:128, :], msg[lo:hi, :], (((1,), (1,)), ((), ())), preferred_element_type=F32)
        out[0, 0, 0, :, lo:hi] = upd.astype(BF16)


def body(coeffs, halo_rows, edge_source, edge_target, edge_count, block_count, wigner, w_zero, w_one, w_two, attn_vector):
    vm = pl.BlockSpec(memory_space=pltpu.VMEM)
    sm = pl.BlockSpec(memory_space=pltpu.SMEM)
    hb = pl.BlockSpec(memory_space=pl.ANY)
    nops = sum(len(chunk_ops(k, r)) for k, (_, _, r) in enumerate(CHUNKS))
    V = pltpu.VMEM
    return pl.pallas_call(
        merged_kernel,
        out_shape=jax.ShapeDtypeStruct((1, 1, 1, 128, 3200), BF16),
        in_specs=[sm, sm] + [hb] * 9,
        out_specs=vm,
        scratch_shapes=[
            V((4, 128), jnp.int32), V((4, 128), jnp.int32), V((1, 32), jnp.int32), V((1, 128), F32), V((128, 3200), BF16), V((165, 4, 128), BF16), V((2, 640, 640), BF16), V((2, 2, 512, 512), BF16), V((2, 2, 384, 384), BF16),
            V((896, 3200), BF16), V((288, 3200), BF16), V((3200, 1024), BF16), V((115, 8, NE), F32),
            V((2, 640, 640), BF16), V((2, 1024, 1024), BF16), V((2, 768, 768), BF16),
            V((1024, NE), BF16), V((9 * CH, NE), F32), V((19 * CH, NE), BF16), V((19 * CH, NE), BF16), V((19 * CH, NE), BF16),
            V((25 * CH, NE), BF16), V((CH, NE), F32), V((CH, NE), F32), V((19 * CH, NE), F32),
            pltpu.SemaphoreType.DMA((9,)), pltpu.SemaphoreType.DMA((nops,)), pltpu.SemaphoreType.DMA((nops,)),
        ],
        compiler_params=pltpu.CompilerParams(vmem_limit_bytes=67043328, collective_id=0, has_side_effects=True),
    )(edge_count, block_count, edge_source, edge_target, halo_rows, attn_vector.reshape(1, 128), coeffs, jnp.transpose(wigner, (0, 1, 2, 4, 3, 5)), w_zero, w_one, w_two)


def solution(mesh):
    placed = (P("gx", "gy", "gz", None, None), P("gx", "gy", "gz", None), P("gx", "gy", "gz", None, None), P("gx", "gy", "gz", None, None),
              P("gx", "gy", "gz", None), P("gx", "gy", "gz"), P("gx", "gy", "gz", None, None, None), P(), P(), P(), P())
    return jax.shard_map(body, mesh=mesh, in_specs=placed, out_specs=P("gx", "gy", "gz", None, None), check_vma=False)
```

```python
import math
import functools
import jax, jax.numpy as jnp, numpy as np
from jax import lax
from jax.experimental import pallas as pl
from jax.experimental.pallas import tpu as pltpu
from jax.sharding import PartitionSpec as P

CH = 128
F32 = jnp.float32
BF16 = jnp.bfloat16
STARTS = [0, 1, 10, 35, 84]
ORDER = [0, 2, 6, 12, 20, 3, 7, 13, 21, 1, 5, 11, 19, 8, 14, 22, 4, 10, 18]
ROWS = []
for l in range(5):
    rows = []
    for pos, comp in enumerate(ORDER):
        if math.isqrt(comp) == l:
            off = comp - l * l
            rows.append((pos, [STARTS[l] + off * (2 * l + 1) + j for j in range(2 * l + 1)]))
    ROWS.append(rows)
USED = sorted({p for rows in ROWS for _, ps in rows for p in ps})
SLOT = {p: i for i, p in enumerate(USED)}
NE = 512


def rotate_out(l, e4, wei, wb, msg):
    d = 2 * l + 1
    for e in (e4 * 128,):
        for c in range(0, CH, 16):
            w = [wei[pos * CH + c:pos * CH + c + 16, e:e + 128].astype(F32) for pos, _ in ROWS[l]]
            for j in range(d):
                acc = [None, None]
                for n, (pos, ps) in enumerate(ROWS[l]):
                    f = wb[SLOT[ps[j]], :, e:e + 128]
                    for h in range(2):
                        t = f * w[n][8 * h:8 * h + 8]
                        acc[h] = t if acc[h] is None else acc[h] + t
                r = (l * l + j) * CH + c
                msg[r:r + 16, e:e + 128] = jnp.concatenate(acc, axis=0).astype(BF16)


def dot(a, b):
    return jnp.dot(a, b, preferred_element_type=F32)


P_S, P_O, P_YO, P_L, P_R, P_YC = range(6)
LINKS = ("right", "left", "yt", "zp", "zm", "partner")
CHUNKS = ((16, 6, 'B'), (22, 3, 'A'), (9, 3, 'B'), (12, 4, 'B'), (4, 5, 'A'), (0, 4, 'B'))
GROUPS = (((0, 1), (4,)), ((2, 3), (3,)), ((4,), (2,)), ((5,), (1, 0)))
RPOS = (15, 16, 0, 1, 2, 17, 3, 4, 5, 18, 6, 7, 8, 9, 10, 11, 12, 13, 14)
KZ = (3, 4, 0, 1, 2)
KP = (6, 0, 1, 2)
KN = (7, 3, 4, 5)


def geometry(gx, gy, gz, div, rem):
    y, xh, xl, c = div(gx, 2), rem(gx, 2), div(gy, 2), rem(gy, 2)
    xor = lambda a, b: a + b - 2 * a * b
    dev = dict(
        right=(y * 2 + xor(xh, xl), 2 * (1 - xl) + c, gz),
        left=(y * 2 + xor(xh, 1 - xl), 2 * (1 - xl) + c, gz),
        yt=(rem(y + 5 - 2 * xh, 4) * 2 + xh, gy, gz),
        ys=(rem(y + 3 + 2 * xh, 4) * 2 + xh, gy, gz),
        zp=(gx, gy, rem(gz + 1, 8)),
        zm=(gx, gy, rem(gz + 7, 8)),
        partner=(gx, 2 * xl + 1 - c, gz),
    )
    dev["relay"] = tuple(a * (1 - c) + b * c for a, b in zip(dev["right"], dev["left"]))
    s, t = 1 - 2 * xh, 1 - 2 * c
    blocks = []
    for q in range(27):
        if q < 9:
            da, db = (0, s, -s)[q // 3], 0
        else:
            p = (q - 9) // 3
            da = (0, s, -s, (1 - xl) * s, xl * s, -s)[p]
            db = (t, t, t, -t, -t, -t)[p]
        blocks.append((da + 1) * 9 + (db + 1) * 3 + q % 3)
    return dev, c, xl, blocks


def chunk_ops(k, route):
    ops = []
    S, O, YO, L, R, YC = (3 * p for p in range(6))
    dks = (1, 0, 2) if route == "A" else (1,)
    if route == "A":
        ops.append((k, "zp", S + 1, S + 0, ()))
        ops.append((k, "zm", S + 1, S + 2, ()))
    for d in dks:
        pre = () if d == 1 else ((k, S + d),)
        ops.append((k, "right", S + d, L + d, pre))
        ops.append((k, "left", S + d, R + d, pre))
    for d in dks:
        ops.append((k, "relay", "F%d" % d, O + d, ((k, L + d), (k, R + d))))
    for d in dks:
        ops.append((k, "yt", "C%d" % d, YC + d, ((k, L + d), (k, R + d))))
        ops.append((k, "yt", O + d, YO + d, ((k, O + d),)))
    if route == "B":
        for p in range(6):
            pre = () if p == 0 else ((k, 3 * p + 1),)
            ops.append((k, "zp", 3 * p + 1, 3 * p + 0, pre))
            ops.append((k, "zm", 3 * p + 1, 3 * p + 2, pre))
    for p in range(6):
        pre = tuple((k, 3 * p + d) for d in range(3) if not (p == 0 and d == 1))
        ops.append((k, "partner", 3 * p, 100 + 3 * p, pre))
    return ops


def plan(pieces, lat=2.4, rate=46.6e3, window=0.3):
    ops = [op for k, (_, _, r) in enumerate(CHUNKS) for op in chunk_ops(k, r)]
    group_of = {k: g for g, (ks, _) in enumerate(GROUPS) for k in ks}
    pend = sorted(ops, key=lambda op: group_of[op[0]])
    free, arrive, seq, now = {}, {}, [], 0.0
    pieces = list(pieces)

    def group_ready(g):
        if g < 0:
            return 0.0
        keys = [(k, 100 + 3 * p) for k in GROUPS[g][0] for p in range(6)]
        return max(arrive.get(key, 1e9) for key in keys)

    def link(op):
        return "right" if op[1] == "relay" else op[1]

    while pend or pieces:
        open_at = [max([arrive.get(x, 1e9) for x in op[4]] + [free.get(link(op), 0.0) - window]) for op in pend]
        ready = [op for op, t in zip(pend, open_at) if t <= now]
        if ready:
            op = ready[0]
            pend.remove(op)
            seq.append(("op", op))
            k, name, _, dst, _ = op
            size = 32 * CHUNKS[k][1] * 256 * (3 if name == "partner" else 1)
            r = 300e3 if name == "partner" else rate * (1.33 if link(op) == "right" else 1.0)
            start = max(now, free.get(link(op), 0.0))
            free[link(op)] = start + size / r
            arrive[(k, dst)] = free[link(op)] + (1.0 if name == "partner" else lat)
            now += 0.02
            continue
        if pieces and group_ready(pieces[0][2]) <= now:
            name, us, _ = pieces.pop(0)
            seq.append(("piece", name))
            now += us
            continue
        now = max(now, min(open_at + [group_ready(p[2]) for p in pieces[:1]]))
    return seq, now, arrive


EPS = 1e-06
NK = len(CHUNKS)


def make_pieces():
    pieces = [("own", 0.7, -1), ("onehot", 0.4, -1)]
    pieces += [("frames%d" % g, 0.15, -1) for g in range(4)]
    pieces += [("weights%d" % i, 0.3, -1) for i in range(10)]
    for gi, (_, degrees) in enumerate(GROUPS):
        lo, hi = degrees[-1] ** 2, (degrees[0] + 1) ** 2
        last = gi == len(GROUPS) - 1
        step = hi - lo if last else 2
        if last:
            pieces += [("early%d" % i, 0.3, -1) for i in range(8)]
        j = lo
        while j < hi:
            n = min(step, hi - j)
            pieces.append(("gather%d:%d:%d:%d" % (gi, j, n, lo), 0.22 * n, gi))
            j += n
        for l in degrees:
            for e in range(4):
                pieces.append(("rotate%d:%d:%d" % (l, e, lo), 0.005 * (2 * l + 1) * min(5, 2 * l + 1), gi))
    return pieces


def rotate_tile(l, e, base, gl, wb, rot):
    d = 2 * l + 1
    e0 = e * 128
    for c in range(0, CH, 16):
        g = [[gl[(base + j) * CH + c + 8 * h:(base + j) * CH + c + 8 * h + 8, e0:e0 + 128] for h in range(2)] for j in range(d)]
        for pos, ps in ROWS[l]:
            acc = [None, None]
            for j in range(d):
                f = wb[SLOT[ps[j]], :, e0:e0 + 128]
                for h in range(2):
                    t = f * g[j][h]
                    acc[h] = t if acc[h] is None else acc[h] + t
            r = RPOS[pos] * CH + c
            rot[r:r + 16, e0:e0 + 128] = jnp.concatenate(acc, axis=0).astype(BF16)


def weight_blocks():
    todo = []
    for v in range(2):
        todo += [(v, 0, a, b) for a in range(5) for b in range(5)]
        todo += [(v, 1, a, b) for a in range(4) for b in range(4)]
        todo += [(v, 2, a, b) for a in range(3) for b in range(3)]
    return todo


def build_block(v, m, a, b, raw, built):
    src, dst, n = raw[m], built[m], (5, 4, 3)[m]
    blk = lambda i: slice(i * CH, (i + 1) * CH)
    if m == 0:
        dst[v, blk(b), blk(a if v else KZ[a])] = src[v, blk(a), blk(b)].T
        return
    p, q = (KP[a], KN[a]) if m == 1 and v == 0 else (a, n + a)
    s, t = (2 * b, 2 * b + 1) if v else (b, n + b)
    re, im = src[v, 0, blk(a), blk(b)].T, src[v, 1, blk(a), blk(b)].T
    dst[v, blk(s), blk(p)] = re
    dst[v, blk(t), blk(q)] = re
    dst[v, blk(s), blk(q)] = -im
    dst[v, blk(t), blk(p)] = im


def early_conv(i, rot, wzt, w1t, w2t, hid):
    if i == 0:
        hid[0:640, :] = dot(wzt[0, :, 0:384], rot[0:384, :])
    elif i < 5:
        b = i - 1
        hid[640 + b * 256:896 + b * 256, :] = dot(w1t[0, b * 256:(b + 1) * 256, 0:768], rot[384:1152, :])
    else:
        b = i - 5
        hid[1664 + b * 256:1920 + b * 256, :] = dot(w2t[0, b * 256:(b + 1) * 256, :], rot[1152:1920, :])


def merged_kernel(cnt, blocks, src_h, tgt_h, halo_h, attn_h, coeffs, wig_h, wz_h, w1_h, w2_h, out,
                  src, tgt, halo, attn, cf, wig, wzr, w1r, w2r, tab, tabo, tabt, wb, wzt, w1t, w2t,
                  oh, gl, rot, act, wei, msg, attb, sigs, hid, obuf, osem, lsem, ssem, rsem):
    MESH = pl.DeviceIdType.MESH
    gx, gy, gz = (lax.axis_index(n) for n in ("gx", "gy", "gz"))
    dev, core, xl, bids = geometry(gx, gy, gz, lax.div, lax.rem)

    loads = [pltpu.make_async_copy(a, b, lsem.at[i]) for i, (a, b) in enumerate(
        ((halo_h.at[0, 0], halo), (coeffs.at[0, 0, 0], cf), (src_h.at[0, 0, 0], src), (tgt_h.at[0, 0, 0], tgt), (attn_h, attn),
         (wig_h.at[0, 0, 0], wig), (wz_h, wzr), (w1_h, w1r), (w2_h, w2r)))]
    for cp in loads:
        cp.start()
    barrier = pltpu.get_barrier_semaphore()
    near = ("right", "left", "yt", "ys", "zp", "zm", "partner")
    for n in near:
        pl.semaphore_signal(barrier, inc=1, device_id=dev[n], device_id_type=MESH)

    loads[0].wait()
    pick = jnp.where(lax.broadcasted_iota(jnp.int32, (128, 32), 0) == halo[...], 1.0, 0.0).astype(F32).T.astype(BF16)
    loads[1].wait()
    rows = dot(pick, cf[...])
    rows = rows * lax.rsqrt(jnp.mean(rows * rows, axis=-1, keepdims=True) + EPS)
    tab[32:64, :] = rows.astype(BF16)
    tab[864:896, :] = jnp.zeros((32, 3200), BF16)
    pl.semaphore_wait(barrier, len(near))

    descs = {}

    def issue(op):
        k, link, s, d, _ = op
        j0, n, _ = CHUNKS[k]
        cols = pl.ds(j0 * CH, n * CH)
        cnt_slots = 3 if link == "partner" else 1
        if isinstance(s, str):
            sel = core if s[0] == "F" else xl
            row = pl.multiple_of((3 * sel + int(s[1])) * 32, 32)
            sref = tabo.at[pl.ds(row, 32), cols]
        elif s < 9:
            sref = tab.at[pl.ds(32 * s, 32 * cnt_slots), cols]
        else:
            sref = tabo.at[pl.ds(32 * (s - 9), 32 * cnt_slots), cols]
        if d >= 100:
            dref = tab.at[pl.ds(288 + 32 * (d - 100), 96), cols]
        elif d < 9:
            dref = tab.at[pl.ds(32 * d, 32), cols]
        else:
            dref = tabo.at[pl.ds(32 * (d - 9), 32), cols]
        i = len(descs)
        cp = pltpu.make_async_remote_copy(src_ref=sref, dst_ref=dref, send_sem=ssem.at[i], recv_sem=rsem.at[i],
                                          device_id=dev[link], device_id_type=MESH)
        descs[(k, d)] = cp
        return cp

    waited = set()

    def arrive(key):
        if key not in waited:
            waited.add(key)
            descs[key].wait_recv()

    raw, built = (wzr, w1r, w2r), (wzt, w1t, w2t)
    wblocks = weight_blocks()

    def piece(name):
        if name == "own":
            x = cf[...].astype(F32)
            f = lax.rsqrt(jnp.mean(x * x, axis=-1, keepdims=True) + EPS)
            for j in range(25):
                tabt[j * CH:(j + 1) * CH, 0:128] = (cf[:, j * CH:(j + 1) * CH].astype(F32) * f).astype(BF16).T
        elif name == "onehot":
            for cp in loads[2:5]:
                cp.wait()
            own = lax.broadcasted_iota(jnp.int32, (128, 128), 0)
            for g in range(4):
                oh[0:128, g * 128:(g + 1) * 128] = jnp.where(own == src[g:g + 1, :], 1.0, 0.0).astype(BF16)
                for q in range(27):
                    at = lax.broadcasted_iota(jnp.int32, (32, 128), 0) + (128 + 32 * bids[q])
                    oh[128 + 32 * q:160 + 32 * q, g * 128:(g + 1) * 128] = jnp.where(at == src[g:g + 1, :], 1.0, 0.0).astype(BF16)
                oh[992:1024, g * 128:(g + 1) * 128] = jnp.zeros((32, 128), BF16)
        elif name.startswith("frames"):
            g = int(name[6:])
            if g == 0:
                loads[5].wait()
            for i, p in enumerate(USED):
                wb[i, :, g * 128:(g + 1) * 128] = jnp.broadcast_to(wig[p, g:g + 1, :].astype(F32), (8, 128))
        elif name.startswith("weights"):
            i = int(name[7:])
            if i == 0:
                for cp in loads[6:]:
                    cp.wait()
            for blk in wblocks[i * 10:(i + 1) * 10]:
                build_block(*blk, raw, built)
        elif name.startswith("gather"):
            gi, j0, n, lo = (int(v) for v in name[6:].split(":"))
            for j in range(j0, j0 + n):
                for g in range(7):
                    tabt[j * CH:(j + 1) * CH, 128 + g * 128:256 + g * 128] = tab[g * 128:(g + 1) * 128, j * CH:(j + 1) * CH].T
            gl[(j0 - lo) * CH:(j0 - lo + n) * CH, :] = dot(tabt[j0 * CH:(j0 + n) * CH, :], oh[...])
        elif name.startswith("rotate"):
            l, e, lo = (int(v) for v in name[6:].split(":"))
            rotate_tile(l, e, l * l - lo, gl, wb, rot)
        elif name.startswith("early"):
            early_conv(int(name[5:]), rot, wzt, w1t, w2t, hid)

    got = set()
    seq, _, _ = plan(make_pieces())
    for kind, what in seq:
        if kind == "op":
            for key in what[4]:
                arrive(key)
            issue(what).start()
        else:
            if what[:6] == "gather":
                g = int(what[6:].split(":")[0])
                if g not in got:
                    got.add(g)
                    for k in GROUPS[g][0]:
                        for p in range(6):
                            arrive((k, 100 + 3 * p))
            piece(what)
    for key, cp in descs.items():
        arrive(key)
        cp.wait_send()

    finish(tgt, cnt, blocks, attn, wb, wzt, w1t, w2t, out, oh, rot, act, wei, msg, attb, sigs, hid, obuf, osem)


def finish(tgt, cnt, blocks, attn_ref, wb, wzt, w1t, w2t, out, oh, rot, act, wei, msg, attb, sigs, hid, obuf, osem):
    attn = jnp.broadcast_to(attn_ref[...], (128, 128)).T

    def emit1(c0, n, val):
        if c0 == 0:
            sig = jax.nn.sigmoid(val)
            sigs[...] = sig
            silu = val * sig
            act[0:128, :] = silu.astype(BF16)
            for g in range(4):
                t = (silu[:, g * 128:(g + 1) * 128] * attn).reshape(8, 16, 128)
                logit = jnp.sum(t, axis=1)
                edge = lax.broadcasted_iota(jnp.int32, (8, 128), 1)
                live = jnp.logical_and(edge < cnt[0, 0, 0, g], g < blocks[0, 0, 0])
                a = jnp.where(live, jax.nn.sigmoid(logit), 0.0)
                attb[:, g * 128:(g + 1) * 128] = jnp.broadcast_to(a[:, None, :], (8, 16, 128)).reshape(128, 128)
        else:
            for k in range(n):
                act[(c0 + k) * CH:(c0 + k + 1) * CH, :] = (val[k * CH:(k + 1) * CH] * sigs[...]).astype(BF16)
    z = rot[15 * CH:17 * CH, :]
    for c0, n in ((0, 1), (1, 2), (3, 2)):
        emit1(c0, n, hid[c0 * CH:(c0 + n) * CH, :] + dot(wzt[0, c0 * CH:(c0 + n) * CH, 384:640], z))
    one = rot[17 * CH:19 * CH, :]
    for b in range(4):
        emit1(5 + 2 * b, 2, hid[640 + b * 256:896 + b * 256, :] + dot(w1t[0, b * 256:(b + 1) * 256, 768:1024], one))
    for b in range(3):
        emit1(13 + 2 * b, 2, hid[1664 + b * 256:1920 + b * 256, :])

    for g in range(4):
        atom = lax.broadcasted_iota(jnp.int32, (128, 128), 0)
        oh[0:128, g * 128:(g + 1) * 128] = jnp.where(atom == tgt[g:g + 1, :], 1.0, 0.0).astype(BF16)

    def mix(l, m):
        if m == 0:
            val = dot(wzt[1, l * CH:(l + 1) * CH, :], act[0:640, :])
            places = (l,)
        elif m == 1:
            val = dot(w1t[1, (l - 1) * 256:l * 256, :], act[640:1664, :])
            places = (4 + l, 8 + l)
        else:
            val = dot(w2t[1, (l - 2) * 256:(l - 1) * 256, :], act[1664:2432, :])
            places = (11 + l, 14 + l)
        for i, pos in enumerate(places):
            wei[pos * CH:(pos + 1) * CH, :] = (val[i * CH:(i + 1) * CH] * attb[...]).astype(BF16)

    def scatter(l):
        lo, hi = l * l * CH, (l + 1) * (l + 1) * CH
        upd = lax.dot_general(oh[0:128, :], msg[lo:hi, :], (((1,), (1,)), ((), ())), preferred_element_type=F32)
        obuf[:, lo:hi] = upd.astype(BF16)
        cp = pltpu.make_async_copy(obuf.at[:, pl.ds(lo, hi - lo)], out.at[0, 0, 0, :, pl.ds(lo, hi - lo)], osem.at[l])
        cp.start()
        return cp

    for m in range(3):
        mix(4, m)
    writes = []
    for l in (4, 3, 2, 1, 0):
        todo = [(l - 1, m) for m in range(min(l, 3))] if l else []
        for e in range(4):
            if todo:
                mix(*todo.pop(0))
            rotate_out(l, e, wei, wb, msg)
        writes.append(scatter(l))
    for cp in writes:
        cp.wait()


def body(coeffs, halo_rows, edge_source, edge_target, edge_count, block_count, wigner, w_zero, w_one, w_two, attn_vector):
    sm = pl.BlockSpec(memory_space=pltpu.SMEM)
    hb = pl.BlockSpec(memory_space=pl.ANY)
    nops = sum(len(chunk_ops(k, r)) for k, (_, _, r) in enumerate(CHUNKS))
    V = pltpu.VMEM
    return pl.pallas_call(
        merged_kernel,
        out_shape=jax.ShapeDtypeStruct((1, 1, 1, 128, 3200), BF16),
        in_specs=[sm, sm] + [hb] * 9,
        out_specs=hb,
        scratch_shapes=[
            V((4, 128), jnp.int32), V((4, 128), jnp.int32), V((1, 32), jnp.int32), V((1, 128), F32), V((128, 3200), BF16), V((165, 4, 128), BF16), V((2, 640, 640), BF16), V((2, 2, 512, 512), BF16), V((2, 2, 384, 384), BF16),
            V((896, 3200), BF16), V((288, 3200), BF16), V((3200, 1024), BF16), V((115, 8, NE), F32),
            V((2, 640, 640), BF16), V((2, 1024, 1024), BF16), V((2, 768, 768), BF16),
            V((1024, NE), BF16), V((9 * CH, NE), F32), V((19 * CH, NE), BF16), V((19 * CH, NE), BF16), V((19 * CH, NE), BF16),
            V((25 * CH, NE), BF16), V((CH, NE), F32), V((CH, NE), F32), V((19 * CH, NE), F32), V((128, 3200), BF16), pltpu.SemaphoreType.DMA((5,)),
            pltpu.SemaphoreType.DMA((9,)), pltpu.SemaphoreType.DMA((nops,)), pltpu.SemaphoreType.DMA((nops,)),
        ],
        compiler_params=pltpu.CompilerParams(vmem_limit_bytes=67043328, collective_id=0, has_side_effects=True),
    )(edge_count, block_count, edge_source, edge_target, halo_rows, attn_vector.reshape(1, 128), coeffs, jnp.transpose(wigner, (0, 1, 2, 4, 3, 5)), w_zero, w_one, w_two)


def solution(mesh):
    placed = (P("gx", "gy", "gz", None, None), P("gx", "gy", "gz", None), P("gx", "gy", "gz", None, None), P("gx", "gy", "gz", None, None),
              P("gx", "gy", "gz", None), P("gx", "gy", "gz"), P("gx", "gy", "gz", None, None, None), P(), P(), P(), P())
    return jax.shard_map(body, mesh=mesh, in_specs=placed, out_specs=P("gx", "gy", "gz", None, None), check_vma=False)
```
